512 devices in a mesh: box: 2 (over y), gx: 128 (over z, x), gy: 2 (over core).
Axes of the slice: x: 8, y: 2, z: 16, core: 2. Of those that a mesh axis runs over, the one named last changes fastest.
The devices are a block of a 8x8x16 slice.
Arguments:
- positions: float32 [256, 4, 3, 256], P(('box', 'gx'), 'gy'), parts along dimension 0, may hold values from 0 to 18, as said below
- polarizability: float32 [256, 4, 256], P(('box', 'gx'), 'gy'), parts along dimension 0, may hold values from 0.3 to 1.5
- tile_counts: int32 [256, 4, 2], P(('box', 'gx'), 'gy'), parts along dimension 0, may hold values from 80 to 128, as said below
- molecules: int32 [256, 4, 256], P(('box', 'gx'), 'gy'), parts along dimension 0, may hold values from 0 to 170, as said below
- perm_field: float32 [256, 4, 3, 256], P(('box', 'gx'), 'gy'), parts along dimension 0, may hold values from -6 to 6
- dipoles: float32 [256, 4, 3, 256], P(('box', 'gx'), 'gy'), parts along dimension 0, may hold values from -4 to 4
- past_out: float32 [256, 4, 7, 3, 256], P(('box', 'gx'), 'gy'), parts along dimension 0, may hold values from -4 to 4
- past_res: float32 [256, 4, 7, 3, 256], P(('box', 'gx'), 'gy'), parts along dimension 0, may hold values from -15 to 15
Outputs:
- dipoles_next: float32 [256, 4, 3, 256], P(('box', 'gx'), 'gy'), parts along dimension 0
- diis_weights: float32 [16], P('box'), parts along dimension 0
The draws below stay inside these ranges and needn't reach their ends.
There are 2 independent parts, one for each index of `box`. The reference program is written for one: setup_inputs(seed, part) draws one part's arguments, and reference() takes and returns one part's arrays. A program takes and returns all parts, laid end to end along the dimension named above; each array names one. Nothing has to cross between parts.
Inputs may be any that keep to these rules, and one draw needn't show every extreme that they name: x and y in [0, 9); z of an atom in z-tile t lies in [9 t, 9 t + 9); padded slots carry positions too. `tile_counts`: some z-tile is full. `molecules`: a group holds at most three atoms, all of one z-tile of one cell.
All inputs are finite; a program needn't handle non-finite values.
Results may differ from the reference program's by a relative error of at most 0.0003.
Values sent between devices are 32-bit elements; how exact they have to be, the bound alone decides.
No kernel may reach another device: no remote copies, remote signals or barrier semaphores. Data moves between devices by JAX's collectives and lax.ppermute only.
A program may use at most 64 MiB of HBM per device.

```python
import math
import jax
import jax.numpy as jnp
from jax import lax

TILE = 128
TILES = 2
HIST = 8
ITERS = 2
ATOMS = 256
CX = 128
CY = 4


def draw_positions(key, part):
    key_plane, key_height = jax.random.split(jax.random.fold_in(key, 11))
    plane_xy = jax.random.uniform(key_plane, (CX, CY, 2, ATOMS), jnp.float32, 0.0, 9.0)
    height = jax.random.uniform(key_height, (CX, CY, 1, ATOMS), jnp.float32, 0.0, 9.0)
    floor_z = (lax.broadcasted_iota(jnp.int32, (CX, CY, 1, ATOMS), 3) // TILE).astype(jnp.float32) * 9.0
    return jnp.concatenate([plane_xy, height + floor_z], axis=2)


def draw_tile_counts(key, part):
    key_fill, key_full = jax.random.split(jax.random.fold_in(key, 23))
    counts = jax.random.randint(key_fill, (CX * CY * TILES,), TILE - 3 * TILE // 8, TILE + 1)
    full_at = jax.random.randint(key_full, (), 0, CX * CY * TILES)
    return counts.at[full_at].set(TILE).reshape(CX, CY, TILES).astype(jnp.int32)


def draw_molecules(key, part):
    dims_all = (CX, CY, TILES, TILE)
    scores = jax.random.randint(jax.random.fold_in(key, 37), dims_all, 0, 1 << 20)
    scores = scores * TILE + lax.broadcasted_iota(jnp.int32, dims_all, 3)
    shuffled = jnp.argsort(scores, axis=3, stable=True).astype(jnp.int32)
    tile_base = lax.broadcasted_iota(jnp.int32, dims_all, 2) * TILE
    return (tile_base + shuffled // 3).reshape(CX, CY, ATOMS)


def draw_past_res(key, part):
    key_private = jax.random.fold_in(jax.random.fold_in(key, 41), 0)
    dims_all = (CX, CY, HIST - 1, 3, ATOMS)
    along_x = lax.broadcasted_iota(jnp.float32, dims_all, 0) / max(CX - 1, 1)
    values = 3.0 ** along_x * jnp.clip(jax.random.normal(key_private, dims_all, jnp.float32), -4.0, 4.0)
    return jnp.clip(values, -15.0, 15.0)


def block_levels(stream_key, shape, cuts, least, high):
    level = 1.0
    for dim, parts in cuts:
        steps = jax.random.uniform(jax.random.fold_in(jax.random.fold_in(stream_key, 6), dim), (parts,), jnp.float32, least / len(cuts), high / len(cuts))
        level = level * jnp.repeat(jnp.exp(steps), shape[dim] // parts).reshape((-1,) + (1,) * (len(shape) - 1 - dim))
    return level


def gaussian(own_key, dims, spread, most, cuts=(), held_as=jnp.bfloat16):
    values = spread * jax.random.normal(own_key, dims, jnp.float32)
    if cuts:
        values = values * block_levels(own_key, dims, cuts, -0.22, 0.18)
    return jnp.clip(values, -most, most).astype(held_as)


def setup_inputs(seed: int = 0, part: int = 0) -> dict:
    seeds = jax.random.split(jax.random.key(seed), 9)
    part_splits = jax.random.split(jax.random.fold_in(seeds[8], part), 9)
    return {
        "positions": draw_positions(jax.random.fold_in(jax.random.fold_in(seeds[8], part), 71), part),
        "polarizability": jnp.clip(jnp.exp(math.log(1.5) - 1.60943787 * jax.random.uniform(part_splits[1], (CX, CY, ATOMS), jnp.float32) ** block_levels(part_splits[1], (CX, CY, ATOMS), ((0, 128), (1, 2)), -0.2, 0.2)), 0.3, 1.5),
        "tile_counts": draw_tile_counts(jax.random.fold_in(jax.random.fold_in(seeds[8], part), 71), part),
        "molecules": draw_molecules(jax.random.fold_in(jax.random.fold_in(seeds[8], part), 71), part),
        "perm_field": gaussian(part_splits[4], (CX, CY, 3, ATOMS), 1.0, 6.0, ((0, 128), (1, 2)), jnp.float32),
        "dipoles": gaussian(part_splits[5], (CX, CY, 3, ATOMS), 0.5, 4.0, ((0, 128), (1, 2)), jnp.float32),
        "past_out": gaussian(part_splits[6], (CX, CY, HIST - 1, 3, ATOMS), 0.5, 4.0, ((0, 128), (1, 2)), jnp.float32),
        "past_res": draw_past_res(jax.random.fold_in(jax.random.fold_in(seeds[8], part), 71), part),
    }


CELL_SIDE = 9.0
CUTOFF_SQ = 81.0
SOFTENING = 0.25
THOLE_DAMP = 0.39
FAR_LIFT = 1000.0

def pair_terms(target_coords, target_polar, target_groups, target_occupied, source_coords, source_polar, source_groups, source_occupied):
    displace = source_coords[:, None, :] - target_coords[:, :, None]
    square_dist = lax.optimization_barrier(jnp.sum(displace * displace, axis=0)) + SOFTENING
    distance = jnp.sqrt(square_dist)
    cube_dist = square_dist * distance
    damped = THOLE_DAMP * cube_dist / jnp.sqrt(target_polar[:, None] * source_polar[None, :])
    damping = jnp.exp(-damped)
    tapering = jnp.square(jnp.maximum(1.0 - square_dist / CUTOFF_SQ, 0.0))
    keeper = (target_groups[:, None] != source_groups[None, :]).astype(jnp.float32)
    weight = tapering * keeper * target_occupied[:, None] * source_occupied[None, :]
    isotropic = weight * -jnp.expm1(-damped) / cube_dist
    tensorial = 3.0 * weight * (1.0 - (1.0 + damped) * damping) / (cube_dist * square_dist)
    return (displace, isotropic, tensorial)

def field_targets(displace, isotropic, tensorial, source_dipole):
    projected = lax.optimization_barrier(jnp.sum(displace * source_dipole[:, None, :], axis=0))
    return lax.optimization_barrier(jnp.sum(displace * (tensorial * projected)[None], axis=2)) - lax.optimization_barrier(jnp.sum(isotropic[None] * source_dipole[:, None, :], axis=2))

def tiled(values, filler, tile_count):
    shaped = values.reshape(values.shape[:-1] + (tile_count, values.shape[-1] // tile_count))
    widths = [(0, 0)] * (shaped.ndim - 2) + [(1, 1), (0, 0)]
    return jnp.pad(shaped, widths, constant_values=filler)

def padded_coords(coords, tile_count):
    marker = tiled(jnp.zeros_like(coords), 1.0, tile_count)
    lifted = jnp.array([0.0, 0.0, FAR_LIFT], jnp.float32).reshape(3, 1, 1)
    return tiled(coords, 0.0, tile_count) + marker * lifted

def band_sources(padded, tile_at):
    coords, polarity, groups, occupied, dipole = padded

    def flat_vector(member):
        window_part = lax.dynamic_slice_in_dim(member, tile_at, 3, 2)
        return jnp.transpose(window_part, (1, 0, 2, 3)).reshape(3, -1)

    def flat_scalar(member):
        return lax.dynamic_slice_in_dim(member, tile_at, 3, 1).reshape(-1)
    return (flat_vector(coords), flat_scalar(polarity), flat_scalar(groups), flat_scalar(occupied), flat_vector(dipole))

def band_field(own_cell, padded, tile_count):
    coords, polarity, groups, occupied = own_cell
    tile_width = coords.shape[-1] // tile_count

    def one_tile(tile_at):
        first_slot = tile_at * tile_width
        source_coords, source_polar, source_groups, source_occupied, source_dipole = band_sources(padded, tile_at)
        displace, isotropic, tensorial = pair_terms(lax.dynamic_slice_in_dim(coords, first_slot, tile_width, 1), lax.dynamic_slice_in_dim(polarity, first_slot, tile_width, 0), lax.dynamic_slice_in_dim(groups, first_slot, tile_width, 0), lax.dynamic_slice_in_dim(occupied, first_slot, tile_width, 0), source_coords, source_polar, source_groups, source_occupied)
        return field_targets(displace, isotropic, tensorial, source_dipole)
    fields = lax.map(one_tile, jnp.arange(tile_count, dtype=jnp.int32))
    return jnp.transpose(fields, (1, 0, 2)).reshape(3, -1)

def field_on(positions, polarizability, molecules, occupied, dipole):
    gathered = ([], [], [], [], [])
    for shift_x in (-1, 0, 1):
        for shift_y in (-1, 0, 1):

            def rolled(values):
                return jnp.roll(values, (-shift_x, -shift_y), axis=(0, 1))
            lifted = jnp.array([CELL_SIDE * shift_x, CELL_SIDE * shift_y, 0.0], jnp.float32).reshape(3, 1)
            gathered[0].append(rolled(positions) + lifted)
            gathered[1].append(rolled(polarizability))
            if shift_x == 0 and shift_y == 0:
                gathered[2].append(molecules)
            else:
                gathered[2].append(jnp.full_like(molecules, -1))
            gathered[3].append(rolled(occupied))
            gathered[4].append(rolled(dipole))
    padded = (padded_coords(jnp.stack(gathered[0], 2), TILES), tiled(jnp.stack(gathered[1], 2), 1.0, TILES), tiled(jnp.stack(gathered[2], 2), -1, TILES), tiled(jnp.stack(gathered[3], 2), 0.0, TILES), tiled(jnp.stack(gathered[4], 2), 0.0, TILES))
    cell_total = CX * CY
    flat_padded = tuple((member.reshape((cell_total,) + member.shape[2:]) for member in padded))
    flat_own = tuple((member.reshape((cell_total,) + member.shape[2:]) for member in (positions, polarizability, molecules, occupied)))

    def per_cell(both_parts):
        return band_field(both_parts[0], both_parts[1], TILES)
    fields = lax.map(per_cell, (flat_own, flat_padded))
    return fields.reshape(CX, CY, 3, -1)

def diis_weights(gram_matrix):
    lower = jnp.linalg.cholesky(gram_matrix)
    history = gram_matrix.shape[0]
    forward = []
    for row_at in range(history):
        running = jnp.ones((), gram_matrix.dtype)
        for col_at in range(row_at):
            running = running - lower[row_at, col_at] * forward[col_at]
        forward.append(running / lower[row_at, row_at])
    backward = [None] * history
    for row_at in reversed(range(history)):
        running = forward[row_at]
        for col_at in range(row_at + 1, history):
            running = running - lower[col_at, row_at] * backward[col_at]
        backward[row_at] = running / lower[row_at, row_at]
    solved = jnp.stack(backward)
    return solved / jnp.sum(solved)

def reference(positions, polarizability, tile_counts, molecules, perm_field, dipoles, past_out, past_res):
    slot_index = lax.broadcasted_iota(jnp.int32, (CX, CY, TILES, TILE), 3)
    occupied = (slot_index < tile_counts[:, :, :, None]).astype(jnp.float32).reshape(CX, CY, ATOMS)
    occupied_vec = occupied[:, :, None, :]
    current = dipoles * occupied_vec
    stored_out = jnp.moveaxis(past_out, 2, 0) * occupied_vec
    stored_res = jnp.moveaxis(past_res, 2, 0) * occupied_vec
    scaled = (polarizability * occupied)[:, :, None, :]
    weights = jnp.zeros((HIST,), jnp.float32)
    for step_at in range(ITERS):
        induced = field_on(positions, polarizability, molecules, occupied, current)
        jacobi = scaled * (perm_field + induced)
        residual = jacobi - current
        outputs_all = jnp.concatenate([stored_out, jacobi[None]], 0)
        residual_all = jnp.concatenate([stored_res, residual[None]], 0)
        flattened = residual_all.reshape(HIST, -1)
        gram_matrix = jnp.dot(flattened.astype(jnp.float32), flattened.T.astype(jnp.float32), precision=lax.Precision.HIGHEST, preferred_element_type=jnp.float32)
        weights = diis_weights(gram_matrix)
        current = lax.optimization_barrier(jnp.sum(weights[:, None, None, None, None] * outputs_all, axis=0))
        stored_out = outputs_all[1:]
        stored_res = residual_all[1:]
    return (current, weights)
```

```python
import functools

import jax
import jax.numpy as jnp
from jax import lax
from jax.experimental import pallas as pl
from jax.experimental.pallas import tpu as pltpu
from jax.sharding import Mesh
from jax.sharding import PartitionSpec as P

GX = ("gx_0", "gx_1")
BOX_GX = ("box", "gx_0", "gx_1")
TORUS_Z = 16
TORUS_X = 8

CELL_SIDE = 9.0
CUTOFF_SQ = 81.0
SOFTENING = 0.25
THOLE_DAMP = 0.39
LN2 = 0.6931471805599453

NVEC = 8
ROW_XYZ = 24
ROW_POLAR = 27
ROW_OCC = 28
ROW_PERM = 29
ROWS = 32
COMPS = 16
BLOCKS = 18
CHUNK = 16
F32 = jnp.float32
BF16 = jnp.bfloat16


def vmem():
    return pl.BlockSpec(memory_space=pltpu.VMEM)


def smem():
    return pl.BlockSpec(memory_space=pltpu.SMEM)


def split3(value):
    first = value.astype(BF16)
    rest = value - first.astype(F32)
    second = rest.astype(BF16)
    third = (rest - second.astype(F32)).astype(BF16)
    return first, second, third


def split2(value):
    first = value.astype(BF16)
    return first, (value - first.astype(F32)).astype(BF16)


def pack_kernel(counts, positions, polarity, permanent, dipoles, past_out, packed):
    cells = positions.shape[0]
    slots = positions.shape[-1]
    tile = slots // counts.shape[1]
    slot = lax.broadcasted_iota(jnp.int32, (1, slots), 1)
    for cell in range(cells):
        occ = (slot < counts[cell, 0]).astype(F32)
        for t in range(1, counts.shape[1]):
            inside = (slot - t * tile < counts[cell, t]).astype(F32)
            occ = jnp.where(slot >= t * tile, inside, occ)
        for comp in range(3):
            for k in range(NVEC - 1):
                row = past_out[cell, k, comp : comp + 1, :] * occ
                packed[cell, comp * NVEC + k : comp * NVEC + k + 1, :] = row
            row = dipoles[cell, comp : comp + 1, :] * occ
            packed[cell, comp * NVEC + NVEC - 1 : comp * NVEC + NVEC, :] = row
            centre = 0.5 * CELL_SIDE if comp < 2 else CELL_SIDE
            row = positions[cell, comp : comp + 1, :] - centre
            packed[cell, ROW_XYZ + comp : ROW_XYZ + comp + 1, :] = row
            row = permanent[cell, comp : comp + 1, :]
            packed[cell, ROW_PERM + comp : ROW_PERM + comp + 1, :] = row
        packed[cell, ROW_POLAR : ROW_POLAR + 1, :] = polarity[cell : cell + 1, :]
        packed[cell, ROW_OCC : ROW_OCC + 1, :] = occ


def source_moments(coords, vectors):
    vx, vy, vz = vectors
    dot = coords[0] * vx + coords[1] * vy + coords[2] * vz
    comps = [coords[i] * dot for i in range(3)]
    comps += [coords[i] * vectors[j] for i in range(3) for j in range(3)]
    return comps + [dot, vx, vy, vz]


def fields_of(moments, isotropic, target):
    along = target[0] * moments[13] + target[1] * moments[14] + target[2] * moments[15]
    shared = moments[12] - along
    out = []
    for i in range(3):
        part = moments[i] - target[i] * shared
        for j in range(3):
            part = part - target[j] * moments[3 + 3 * i + j]
        out.append(3.0 * part - isotropic[i])
    return out


def block_of(index, core, cells):
    near = index < 12
    own_at = jnp.maximum(index - 12, 0)
    step = lax.rem(index, 3) - 1
    own_target = 2 * core + own_at // 3
    target = jnp.where(near, lax.rem(index // 3 - step + cells, cells), own_target)
    source = jnp.where(
        near, index // 3, cells + lax.rem(own_target + step + cells, cells)
    )
    side = jnp.where(near, 1 - 2 * core, 0)
    move_x = side.astype(F32) * CELL_SIDE
    move_y = step.astype(F32) * CELL_SIDE
    inside = jnp.logical_and(index >= 12, step == 0)
    return source, target, own_at // 3, inside, move_x, move_y


def moved_target(rows, move_x, move_y):
    return (rows[0:1] - move_x, rows[1:2] - move_y, rows[2:3])


def pair_kernel(column, beside, groups, fields, pairs, moments, sources):
    cells = column.shape[0]
    slots = column.shape[-1]
    core = lax.axis_index("gy")
    for at in range(2 * cells):
        cell = beside[at] if at < cells else column[at - cells]
        coords = [cell[ROW_XYZ + i : ROW_XYZ + i + 1] for i in range(3)]
        vectors = [cell[NVEC * i : NVEC * i + NVEC] for i in range(3)]
        stacked = jnp.concatenate(source_moments(coords, vectors), axis=0)
        for part, value in enumerate(split3(stacked)):
            moments[at, part * COMPS * NVEC : (part + 1) * COMPS * NVEC, :] = value
        scale = lax.rsqrt(cell[ROW_POLAR : ROW_POLAR + 1])
        tail = jnp.concatenate(coords + [scale] + [jnp.zeros((4, slots), F32)], axis=0)
        sources[at] = tail.T
    fields[...] = jnp.zeros(fields.shape, F32)
    group_columns = jnp.concatenate([groups[...].astype(F32), jnp.zeros((6, slots), F32)], 0).T

    def one_block(index, inside_check):
        source, target, own_at, inside, move_x, move_y = block_of(index, core, cells)
        rows = column[target, ROW_XYZ : ROWS, :]
        place = moved_target(rows, move_x, move_y)
        scale = lax.rsqrt(rows[3:4]) * (-THOLE_DAMP / LN2)
        if inside_check:
            group = groups[pl.ds(own_at, 1), :].astype(F32)
            group = jnp.where(inside, group, -1.0)
        for chunk in range(slots // CHUNK):
            part = pl.ds(chunk * CHUNK, CHUNK)
            near = sources[source, part, :]
            dx = near[:, 0:1] - place[0]
            dy = near[:, 1:2] - place[1]
            dz = near[:, 2:3] - place[2]
            square = (dx * dx + dy * dy) + dz * dz + SOFTENING
            inverse = lax.rsqrt(square)
            inverse_sq = inverse * inverse
            inverse_cube = inverse_sq * inverse
            exponent = (square * square * inverse) * (near[:, 3:4] * scale)
            damping = jnp.exp2(exponent)
            taper = jnp.maximum(1.0 - square * (1.0 / CUTOFF_SQ), 0.0)
            weight = taper * taper * inverse_cube
            if inside_check:
                keys = jnp.where(own_at == 0, group_part0[chunk], group_part1[chunk])
                weight = jnp.where(keys == group, 0.0, weight)
            isotropic = weight * (1.0 - damping)
            tensorial = weight * inverse_sq * (1.0 - (1.0 - LN2 * exponent) * damping)
            for at, value in enumerate(split3(tensorial) + split2(isotropic)):
                pairs[index, at, part, :] = value
        lhs = moments[source]
        size = COMPS * NVEC
        first = jnp.dot(lhs, pairs[index, 0], preferred_element_type=F32)
        second = jnp.dot(lhs[: 2 * size], pairs[index, 1], preferred_element_type=F32)
        third = jnp.dot(lhs[:size], pairs[index, 2], preferred_element_type=F32)
        total = (first[:size] + first[size : 2 * size] + first[2 * size :]) + (
            second[:size] + second[size:] + third
        )
        low = size - 4 * NVEC
        iso_lhs = jnp.concatenate([lhs[low:size], lhs[size + low : 2 * size], lhs[2 * size + low :]], 0)
        first = jnp.dot(iso_lhs, pairs[index, 3], preferred_element_type=F32)
        second = jnp.dot(iso_lhs[: 8 * NVEC], pairs[index, 4], preferred_element_type=F32)
        band = 4 * NVEC
        iso = (first[:band] + first[band : 2 * band] + first[2 * band :]) + (
            second[:band] + second[band:]
        )
        result = fields_of(
            [total[NVEC * i : NVEC * i + NVEC] for i in range(COMPS)],
            [iso[NVEC * i : NVEC * i + NVEC] for i in range(1, 4)],
            place,
        )
        for i in range(3):
            fields[target, NVEC * i : NVEC * i + NVEC, :] += result[i]

    group_part0 = [group_columns[c * CHUNK : (c + 1) * CHUNK, 0:1] for c in range(slots // CHUNK)]
    group_part1 = [group_columns[c * CHUNK : (c + 1) * CHUNK, 1:2] for c in range(slots // CHUNK)]

    def near_body(index, carry):
        one_block(index, False)
        return carry

    def own_body(index, carry):
        one_block(index, True)
        return carry

    lax.fori_loop(0, 12, near_body, 0)
    lax.fori_loop(12, BLOCKS, own_body, 0)


def jacobi_kernel(shared, column, jacobi):
    for cell in range(column.shape[0]):
        scaled = column[cell, ROW_POLAR : ROW_POLAR + 1] * column[cell, ROW_OCC : ROW_OCC + 1]
        for i in range(3):
            row = NVEC * i + NVEC - 1
            field = shared[0, cell, row : row + 1] + shared[1, cell, row : row + 1]
            perm = column[cell, ROW_PERM + i : ROW_PERM + i + 1]
            jacobi[cell, i : i + 1, :] = scaled * (perm + field)


def apply_kernel(column, beside, jacobi, jacobi_beside, pairs, fields, moments):
    cells = column.shape[0]
    core = lax.axis_index("gy")
    for at in range(2 * cells):
        cell = beside[at] if at < cells else column[at - cells]
        vector = jacobi_beside[at] if at < cells else jacobi[at - cells]
        coords = [cell[ROW_XYZ + i : ROW_XYZ + i + 1] for i in range(3)]
        vectors = [vector[i : i + 1] for i in range(3)]
        stacked = jnp.concatenate(source_moments(coords, vectors), axis=0)
        for part, value in enumerate(split3(stacked)):
            moments[at, part * COMPS : (part + 1) * COMPS, :] = value
    fields[...] = jnp.zeros(fields.shape, F32)

    def one_block(index, carry):
        source, target, own_at, inside, move_x, move_y = block_of(index, core, cells)
        place = moved_target(column[target, ROW_XYZ : ROWS, :], move_x, move_y)
        lhs = moments[source]
        first = jnp.dot(lhs, pairs[index, 0], preferred_element_type=F32)
        second = jnp.dot(lhs[: 2 * COMPS], pairs[index, 1], preferred_element_type=F32)
        third = jnp.dot(lhs[:COMPS], pairs[index, 2], preferred_element_type=F32)
        total = (first[:COMPS] + first[COMPS : 2 * COMPS] + first[2 * COMPS :]) + (
            second[:COMPS] + second[COMPS:] + third
        )
        first = jnp.dot(lhs, pairs[index, 3], preferred_element_type=F32)
        second = jnp.dot(lhs[: 2 * COMPS], pairs[index, 4], preferred_element_type=F32)
        iso = (first[:COMPS] + first[COMPS : 2 * COMPS] + first[2 * COMPS :]) + (
            second[:COMPS] + second[COMPS:]
        )
        result = fields_of(
            [total[i : i + 1] for i in range(COMPS)],
            [iso[i : i + 1] for i in range(COMPS - 3, COMPS)],
            place,
        )
        for i in range(3):
            fields[target, i : i + 1, :] += result[i]
        return carry

    lax.fori_loop(0, BLOCKS, one_block, 0)


def own_vectors(core, cell, i, column, jacobi, shared, shared_last):
    at = 2 * core + cell
    slots = column.shape[-1]
    last = lax.broadcasted_iota(jnp.int32, (NVEC, slots), 0) == NVEC - 1
    rows = slice(NVEC * i, NVEC * i + NVEC)
    vectors = column[at, rows, :]
    current = vectors[NVEC - 1 :]
    jacobi_row = jacobi[at, i : i + 1, :]
    vectors = jnp.where(last, jacobi_row, vectors)
    field = shared[0, at, rows, :] + shared[1, at, rows, :]
    newest = shared_last[0, at, i : i + 1, :] + shared_last[1, at, i : i + 1, :]
    field = jnp.where(last, newest, field)
    scaled = column[at, ROW_POLAR : ROW_POLAR + 1, :] * column[at, ROW_OCC : ROW_OCC + 1, :]
    perm = column[at, ROW_PERM + i : ROW_PERM + i + 1, :]
    return vectors, field, current, jacobi_row, scaled, perm


def gram_kernel(column, jacobi, shared, shared_last, past_res, gram):
    core = lax.axis_index("gy")
    slots = column.shape[-1]
    last = lax.broadcasted_iota(jnp.int32, (NVEC, slots), 0) == NVEC - 1
    total = jnp.zeros((2 * NVEC, 4 * NVEC * NVEC), F32)
    for cell in range(past_res.shape[0]):
        occ = column[2 * core + cell, ROW_OCC : ROW_OCC + 1, :]
        for i in range(3):
            vectors, field, current, newest, scaled, perm = own_vectors(
                core, cell, i, column, jacobi, shared, shared_last
            )
            old = [past_res[cell, k, i : i + 1, :] for k in range(NVEC - 1)]
            residual = jnp.concatenate(old + [newest - current], axis=0) * occ
            implied = scaled * (perm + field) - vectors
            both = jnp.concatenate([residual, implied], axis=0)
            many = jnp.concatenate([both] * (2 * NVEC), axis=0)
            total = total + lax.dot_general(
                both,
                many,
                (((1,), (1,)), ((), ())),
                precision=lax.Precision.HIGHEST,
                preferred_element_type=F32,
            )
    shape = total.shape
    row = lax.broadcasted_iota(jnp.int32, shape, 0)
    lane = lax.broadcasted_iota(jnp.int32, shape, 1)
    flat = jnp.sum(jnp.where(lane // (2 * NVEC) == row, total, 0.0), axis=0, keepdims=True)
    half = shape[1] // 2
    gram[0:1, :] = flat[:, :half]
    gram[1:2, :] = flat[:, half:]


def solve_ones(matrix):
    size = len(matrix)
    lower = [[None] * size for _ in range(size)]
    inverse = [None] * size
    scaled = [[None] * size for _ in range(size)]
    for j in range(size):
        for i in range(j, size):
            value = matrix[i][j]
            for k in range(j):
                value = value - scaled[i][k] * lower[j][k]
            scaled[i][j] = value
        inverse[j] = 1.0 / scaled[j][j]
        for i in range(j + 1, size):
            lower[i][j] = scaled[i][j] * inverse[j]
    forward = []
    for i in range(size):
        value = jnp.ones_like(inverse[0])
        for k in range(i):
            value = value - lower[i][k] * forward[k]
        forward.append(value)
    backward = [None] * size
    for i in reversed(range(size)):
        value = forward[i] * inverse[i]
        for k in range(i + 1, size):
            value = value - lower[k][i] * backward[k]
        backward[i] = value
    total = sum(backward[1:], backward[0])
    return [value / total for value in backward]


def finish_kernel(partials, column, jacobi, shared, shared_last, dipoles, weights):
    core = lax.axis_index("gy")
    slots = column.shape[-1]
    lanes = partials.shape[-1]
    summed = partials[0]
    for k in range(1, partials.shape[0]):
        summed = summed + partials[k]

    def entry(k, j):
        flat = k * 2 * NVEC + j
        row, lane = flat // lanes, flat % lanes
        return jnp.broadcast_to(summed[row : row + 1, lane : lane + 1], (1, lanes))

    first = [[entry(j, k) if j <= k else None for j in range(NVEC)] for k in range(NVEC)]
    early = solve_ones(first)
    mixed = []
    for k in range(1, NVEC):
        value = early[0] * entry(k, NVEC)
        for m in range(1, NVEC):
            value = value + early[m] * entry(k, NVEC + m)
        mixed.append(value)
    square = None
    for m in range(NVEC):
        value = 0.5 * early[m] * entry(NVEC + m, NVEC + m)
        for n in range(m + 1, NVEC):
            value = value + early[n] * entry(NVEC + m, NVEC + n)
        value = early[m] * value
        square = value if square is None else square + value
    second = [
        [first[k][j] if j <= k else None for j in range(1, NVEC)] + [None]
        for k in range(1, NVEC)
    ]
    second.append(mixed + [2.0 * square])
    late = solve_ones(second)

    sub = lax.broadcasted_iota(jnp.int32, (NVEC, lanes), 0)
    lane = lax.broadcasted_iota(jnp.int32, (1, lanes), 1)
    early_column = jnp.zeros((NVEC, lanes), F32)
    late_column = jnp.zeros((NVEC, lanes), F32)
    row = jnp.zeros((1, lanes), F32)
    for k in range(NVEC):
        early_column = jnp.where(sub == k, early[k], early_column)
        if k:
            late_column = jnp.where(sub == k, late[k - 1], late_column)
        row = jnp.where(lane == k, late[k], row)
    weights[...] = row
    reach = slots // lanes
    early_column = jnp.concatenate([early_column] * reach, axis=1)
    late_column = jnp.concatenate([late_column] * reach, axis=1)
    last = jnp.concatenate([late[NVEC - 1]] * reach, axis=1)
    for cell in range(dipoles.shape[0]):
        for i in range(3):
            vectors, field, current, newest, scaled, perm = own_vectors(
                core, cell, i, column, jacobi, shared, shared_last
            )
            induced = jnp.sum(early_column * field, axis=0, keepdims=True)
            output = scaled * (perm + induced)
            kept = jnp.sum(late_column * vectors, axis=0, keepdims=True)
            dipoles[cell, i : i + 1, :] = kept + last * output


def call(kernel, out_shape, operands, specs=None, scratch=(), megabytes=16):
    single = not isinstance(out_shape, (list, tuple))
    outs = [out_shape] if single else list(out_shape)
    result = pl.pallas_call(
        kernel,
        out_shape=outs,
        in_specs=specs or [vmem() for _ in operands],
        out_specs=[vmem() for _ in outs],
        scratch_shapes=list(scratch),
        compiler_params=pltpu.CompilerParams(vmem_limit_bytes=megabytes << 20),
    )(*operands)
    return result[0] if single else result


def shape_of(*dims, dtype=F32):
    return jax.ShapeDtypeStruct(dims, dtype)


def sideways(block):
    count = lax.axis_size(GX)
    cores = lax.axis_size("gy")
    route = []
    for x in range(count):
        for core in range(cores):
            source = (x + 1 - 2 * core) % count
            route.append((source * cores + core, x * cores + core))
    return lax.ppermute(block, GX + ("gy",), route)


def exchanged(block, axes):
    size = lax.axis_size(axes)
    many = jnp.broadcast_to(block[None], (size,) + block.shape)
    return lax.all_to_all(many, axes, 0, 0)


def body(
    positions, polarizability, tile_counts, molecules, perm_field, dipoles, past_out, past_res
):
    own_cells, slots = positions.shape[1], positions.shape[-1]
    packed = call(
        pack_kernel,
        shape_of(own_cells, ROWS, slots),
        (tile_counts[0], positions[0], polarizability[0], perm_field[0], dipoles[0], past_out[0]),
        [smem()] + [vmem()] * 5,
    )
    column = lax.all_gather(packed, "gy").reshape(-1, ROWS, slots)
    cells = column.shape[0]
    beside = sideways(column)
    partial, pairs = call(
        pair_kernel,
        [shape_of(cells, 3 * NVEC, slots), shape_of(BLOCKS, 5, slots, slots, dtype=BF16)],
        (column, beside, molecules[0]),
        scratch=[
            pltpu.VMEM((2 * cells, 3 * COMPS * NVEC, slots), BF16),
            pltpu.VMEM((2 * cells, slots, 8), F32),
        ],
        megabytes=48,
    )
    shared = lax.all_gather(partial, "gy")
    jacobi = call(jacobi_kernel, shape_of(cells, 3, slots), (shared, column))
    jacobi_beside = sideways(jacobi)
    partial_last = call(
        apply_kernel,
        shape_of(cells, 3, slots),
        (column, beside, jacobi, jacobi_beside, pairs),
        scratch=[pltpu.VMEM((2 * cells, 3 * COMPS, slots), BF16)],
        megabytes=40,
    )
    shared_last = lax.all_gather(partial_last, "gy")
    gram = call(
        gram_kernel,
        shape_of(2, 2 * NVEC * NVEC),
        (column, jacobi, shared, shared_last, past_res[0]),
    )
    gram = jnp.sum(exchanged(gram, ("gx_1", "gy")), axis=0)
    partials = exchanged(gram, ("gx_0",))
    following, weights = call(
        finish_kernel,
        [shape_of(own_cells, 3, slots), shape_of(1, 2 * NVEC * NVEC)],
        (partials, column, jacobi, shared, shared_last),
    )
    return (following[None], weights[0, :NVEC])


def solution(mesh):
    torus = Mesh(
        mesh.devices.reshape(mesh.shape["box"], TORUS_Z, TORUS_X, mesh.shape["gy"]),
        ("box", "gx_0", "gx_1", "gy"),
    )
    return jax.shard_map(
        body,
        mesh=torus,
        in_specs=(
            P(BOX_GX, "gy", None, None),
            P(BOX_GX, "gy", None),
            P(BOX_GX, "gy", None),
            P(BOX_GX, "gy", None),
            P(BOX_GX, "gy", None, None),
            P(BOX_GX, "gy", None, None),
            P(BOX_GX, "gy", None, None, None),
            P(BOX_GX, "gy", None, None, None),
        ),
        out_specs=(P(BOX_GX, "gy", None, None), P("box")),
        check_vma=False,
    )
```

```python
import functools

import jax
import jax.numpy as jnp
from jax import lax
from jax.experimental import pallas as pl
from jax.experimental.pallas import tpu as pltpu
from jax.sharding import Mesh
from jax.sharding import PartitionSpec as P

GX = ("gx_0", "gx_1")
BOX_GX = ("box", "gx_0", "gx_1")
TORUS_Z = 16
TORUS_X = 8

CELL_SIDE = 9.0
CUTOFF_SQ = 81.0
SOFTENING = 0.25
THOLE_DAMP = 0.39
LN2 = 0.6931471805599453

NVEC = 8
ROW_XYZ = 24
ROW_POLAR = 27
ROW_OCC = 28
ROW_PERM = 29
ROWS = 32
COMPS = 16
CHUNK = 16
F32 = jnp.float32
BF16 = jnp.bfloat16


def vmem():
    return pl.BlockSpec(memory_space=pltpu.VMEM)


def smem():
    return pl.BlockSpec(memory_space=pltpu.SMEM)


def split3(value):
    first = value.astype(BF16)
    rest = value - first.astype(F32)
    second = rest.astype(BF16)
    third = (rest - second.astype(F32)).astype(BF16)
    return first, second, third


def split2(value):
    first = value.astype(BF16)
    return first, (value - first.astype(F32)).astype(BF16)


def pack_kernel(*refs):
    sources, packed, groups = refs[:7], refs[7], refs[8]
    held, semaphores = refs[9:16], refs[16]
    copies = [
        pltpu.make_async_copy(source, target, semaphores.at[at])
        for at, (source, target) in enumerate(zip(sources, held))
    ]
    for copy in copies:
        copy.start()
    for copy in copies:
        copy.wait()
    counts, positions, polarity, molecules, permanent, dipoles, past_out = held
    cells, slots = polarity.shape
    tiles = sources[0].shape[1]
    tile = slots // tiles
    slot = lax.broadcasted_iota(jnp.int32, (1, slots), 1)
    groups[...] = jnp.zeros(groups.shape, F32)
    for cell in range(cells):
        occ = (slot < counts[cell, 0]).astype(F32)
        for t in range(1, tiles):
            inside = (slot - t * tile < counts[cell, t]).astype(F32)
            occ = jnp.where(slot >= t * tile, inside, occ)
        at = slice(cell, cell + 1)
        for comp in range(3):
            for k in range(NVEC - 1):
                row = comp * NVEC + k
                packed[cell, row : row + 1, :] = past_out[k, comp, at, :] * occ
            row = comp * NVEC + NVEC - 1
            packed[cell, row : row + 1, :] = dipoles[comp, at, :] * occ
            centre = 0.5 * CELL_SIDE if comp < 2 else CELL_SIDE
            row = (positions[comp, at, :] - centre) * (1.0 / CELL_SIDE)
            packed[cell, ROW_XYZ + comp : ROW_XYZ + comp + 1, :] = row
            packed[cell, ROW_PERM + comp : ROW_PERM + comp + 1, :] = permanent[comp, at, :]
        packed[cell, ROW_POLAR : ROW_POLAR + 1, :] = polarity[at, :]
        packed[cell, ROW_OCC : ROW_OCC + 1, :] = occ
        groups[at, :] = molecules[at, :].astype(F32)


def source_moments(coords, vectors):
    vx, vy, vz = [v * (1.0 / CELL_SIDE**3) for v in vectors]
    dot = coords[0] * vx + coords[1] * vy + coords[2] * vz
    comps = [coords[i] * dot for i in range(3)]
    comps += [coords[i] * v for i in range(3) for v in (vx, vy, vz)]
    return comps + [dot, vx, vy, vz]


def fields_of(moments, isotropic, target):
    along = target[0] * moments[13] + target[1] * moments[14] + target[2] * moments[15]
    shared = moments[12] - along
    out = []
    for i in range(3):
        part = moments[i] - target[i] * shared
        for j in range(3):
            part = part - target[j] * moments[3 + 3 * i + j]
        out.append(3.0 * part - isotropic[i])
    return out


def beside_block(index, core, cells):
    source, step = index // 3, index % 3 - 1
    return source, (source - step) % cells, 0, (1 - 2 * core).astype(F32), step, False


def column_block(index, core, cells):
    own_at, step = index // 3, index % 3 - 1
    target = 2 * core + own_at
    return lax.rem(target + step + cells, cells), target, own_at, 0.0, step, step == 0


def place_of(column, block):
    _, target, _, move_x, step, _ = block
    x = column[target, ROW_XYZ : ROW_XYZ + 1, :] - move_x
    y = column[target, ROW_XYZ + 1 : ROW_XYZ + 2, :] - float(step)
    return x, y, column[target, ROW_XYZ + 2 : ROW_XYZ + 3, :]


def filled_rows(rows, count):
    slots = rows[0].shape[-1]
    return jnp.concatenate(rows + [jnp.zeros((count - len(rows), slots), F32)], axis=0)


def paired_parts(value, order):
    parts = [part.astype(F32) for part in split3(value)]
    blank = jnp.zeros_like(value)
    return [parts[at] for at in order] + [blank]


def pair_loop(count, block_at, column, groups, fields, even, odd, moments, feats, columns, square):
    cells, slots = column.shape[0], column.shape[-1]
    core = lax.axis_index("gy")

    def info(index):
        return block_at(index, core, cells)

    def distances(index):
        block = info(index)
        x, y, z = place_of(column, block)
        norm = x * x + y * y + z * z
        rows = filled_rows([-2.0 * x, -2.0 * y, -2.0 * z, norm, jnp.ones_like(norm)], 8)
        rhs = jnp.concatenate(
            [jnp.zeros_like(rows)] + paired_parts(rows, (0, 0, 0, 1, 1, 2)), axis=0
        ).astype(BF16)
        square[index] = jnp.dot(feats[block[0]], rhs, preferred_element_type=F32)

    def produce(index, out, at):
        block = info(index)
        source, target, own_at = block[:3]
        scale = lax.rsqrt(column[target, ROW_POLAR : ROW_POLAR + 1, :])
        scale = scale * (-THOLE_DAMP * CELL_SIDE**3 / LN2)
        if block[5]:
            group = groups[own_at : own_at + 1, :]
        for chunk in range(slots // CHUNK):
            part = slice(chunk * CHUNK, (chunk + 1) * CHUNK)
            near = columns[source, part, :]
            squared = square[index, part, :]
            inverse = lax.rsqrt(squared)
            inverse_sq = inverse * inverse
            exponent = (squared * squared * inverse) * (near[:, 0:1] * scale)
            damping = jnp.exp2(exponent)
            taper = jnp.maximum(1.0 - squared, 0.0)
            weight = (taper * taper) * (inverse_sq * inverse)
            if block[5]:
                weight = jnp.where(near[:, 1:2] == group, 0.0, weight)
            undamped = 1.0 - damping
            isotropic = weight * undamped
            tensorial = (weight * inverse_sq) * (undamped + (LN2 * exponent) * damping)
            for k, value in enumerate(split2(tensorial) + split2(isotropic)):
                out[at, k, part, :] = value

    def apply(index, pairs, at):
        block = info(index)
        lhs = moments[block[0]]
        size = COMPS * NVEC
        low, band = size - 4 * NVEC, 4 * NVEC
        first = jnp.dot(lhs, pairs[at, 0], preferred_element_type=F32)
        second = jnp.dot(lhs[:size], pairs[at, 1], preferred_element_type=F32)
        total = first[:size] + first[size:] + second
        iso_lhs = jnp.concatenate([lhs[low:size], lhs[size + low :]], 0)
        first = jnp.dot(iso_lhs, pairs[at, 2], preferred_element_type=F32)
        second = jnp.dot(lhs[low:size], pairs[at, 3], preferred_element_type=F32)
        iso = first[:band] + first[band:] + second
        result = fields_of(
            [total[NVEC * i : NVEC * i + NVEC] for i in range(COMPS)],
            [iso[NVEC * i : NVEC * i + NVEC] for i in range(1, 4)],
            place_of(column, block),
        )
        for i in range(3):
            fields[block[1], NVEC * i : NVEC * i + NVEC, :] += result[i]

    ahead = 2
    for index in range(count + 1):
        for later in range(ahead + 1) if index == 0 else (index + ahead,):
            if later < count:
                distances(later)
        if index < count:
            produce(index, (even, odd)[index % 2], index // 2)
        if index:
            last = index - 1
            apply(last, (even, odd)[last % 2], last // 2)


def load_sources(cells, groups, moments, feats, columns):
    core = lax.axis_index("gy")
    for at in range(cells.shape[0]):
        cell = cells[at]
        coords = [cell[ROW_XYZ + i : ROW_XYZ + i + 1] for i in range(3)]
        vectors = [cell[NVEC * i : NVEC * i + NVEC] for i in range(3)]
        stacked = jnp.concatenate(source_moments(coords, vectors), axis=0)
        for part, value in enumerate(split2(stacked)):
            moments[at, part * COMPS * NVEC : (part + 1) * COMPS * NVEC, :] = value
        norm = coords[0] * coords[0] + coords[1] * coords[1] + coords[2] * coords[2]
        norm = norm + SOFTENING / CELL_SIDE**2
        head = [lax.rsqrt(cell[ROW_POLAR : ROW_POLAR + 1])]
        if groups is not None:
            own = jnp.clip(at - 2 * core, 0, 1)
            head.append(groups[pl.ds(own, 1), :])
        rows = filled_rows(coords + [jnp.ones_like(norm), norm], 8)
        tall = jnp.concatenate(
            [filled_rows(head, 8)] + paired_parts(rows, (0, 1, 2, 0, 1, 0)), axis=0
        ).T
        columns[at] = tall
        feats[at] = tall.astype(BF16)


def own_pairs_kernel(column, groups, fields, even, odd, moments, feats, columns, square):
    fields[...] = jnp.zeros(fields.shape, F32)
    load_sources(column, groups, moments, feats, columns)
    pair_loop(6, column_block, column, groups, fields, even, odd, moments, feats, columns, square)


def beside_pairs_kernel(column, beside, begun, fields, even, odd, moments, feats, columns, square):
    fields[...] = begun[...]
    load_sources(beside, None, moments, feats, columns)
    pair_loop(12, beside_block, column, None, fields, even, odd, moments, feats, columns, square)


def jacobi_kernel(shared, column, jacobi):
    for cell in range(column.shape[0]):
        scaled = column[cell, ROW_POLAR : ROW_POLAR + 1] * column[cell, ROW_OCC : ROW_OCC + 1]
        for i in range(3):
            row = NVEC * i + NVEC - 1
            field = shared[0, cell, row : row + 1] + shared[1, cell, row : row + 1]
            perm = column[cell, ROW_PERM + i : ROW_PERM + i + 1]
            jacobi[cell, i : i + 1, :] = scaled * (perm + field)


def apply_pairs(count, block_at, column, cells, vectors, even, odd, fields, moments):
    core = lax.axis_index("gy")
    for at in range(cells.shape[0]):
        coords = [cells[at, ROW_XYZ + i : ROW_XYZ + i + 1, :] for i in range(3)]
        values = [vectors[at, i : i + 1, :] for i in range(3)]
        stacked = jnp.concatenate(source_moments(coords, values), axis=0)
        for part, value in enumerate(split2(stacked)):
            moments[at, part * COMPS : (part + 1) * COMPS, :] = value
    for index in range(count):
        block = block_at(index, core, cells.shape[0])
        pairs, at = (even, odd)[index % 2], index // 2
        lhs = moments[block[0]]
        first = jnp.dot(lhs, pairs[at, 0], preferred_element_type=F32)
        second = jnp.dot(lhs[:COMPS], pairs[at, 1], preferred_element_type=F32)
        total = first[:COMPS] + first[COMPS:] + second
        first = jnp.dot(lhs, pairs[at, 2], preferred_element_type=F32)
        second = jnp.dot(lhs[:COMPS], pairs[at, 3], preferred_element_type=F32)
        iso = first[:COMPS] + first[COMPS:] + second
        result = fields_of(
            [total[i : i + 1] for i in range(COMPS)],
            [iso[i : i + 1] for i in range(COMPS - 3, COMPS)],
            place_of(column, block),
        )
        for i in range(3):
            fields[block[1], i : i + 1, :] += result[i]


def own_apply_kernel(column, jacobi, even, odd, fields, moments):
    fields[...] = jnp.zeros(fields.shape, F32)
    apply_pairs(6, column_block, column, column, jacobi, even, odd, fields, moments)


def beside_apply_kernel(column, beside, jacobi, even, odd, begun, fields, moments):
    fields[...] = begun[...]
    apply_pairs(12, beside_block, column, beside, jacobi, even, odd, fields, moments)


def own_vectors(core, cell, i, column, jacobi, shared, shared_last):
    at = 2 * core + cell
    slots = column.shape[-1]
    last = lax.broadcasted_iota(jnp.int32, (NVEC, slots), 0) == NVEC - 1
    rows = slice(NVEC * i, NVEC * i + NVEC)
    vectors = column[at, rows, :]
    current = vectors[NVEC - 1 :]
    jacobi_row = jacobi[at, i : i + 1, :]
    vectors = jnp.where(last, jacobi_row, vectors)
    field = shared[0, at, rows, :] + shared[1, at, rows, :]
    newest = shared_last[0, at, i : i + 1, :] + shared_last[1, at, i : i + 1, :]
    field = jnp.where(last, newest, field)
    scaled = column[at, ROW_POLAR : ROW_POLAR + 1, :] * column[at, ROW_OCC : ROW_OCC + 1, :]
    perm = column[at, ROW_PERM + i : ROW_PERM + i + 1, :]
    return vectors, field, current, jacobi_row, scaled, perm


def gram_kernel(column, jacobi, shared, shared_last, past_res, gram):
    core = lax.axis_index("gy")
    pieces = []
    for cell in range(past_res.shape[2]):
        occ = column[2 * core + cell, ROW_OCC : ROW_OCC + 1, :]
        for i in range(3):
            vectors, field, current, newest, scaled, perm = own_vectors(
                core, cell, i, column, jacobi, shared, shared_last
            )
            old = [past_res[k, i, cell : cell + 1, :] for k in range(NVEC - 1)]
            residual = jnp.concatenate(old + [newest - current], axis=0) * occ
            implied = scaled * (perm + field) - vectors
            pieces.append(jnp.concatenate([residual, implied], axis=0))
    count = 2 * NVEC
    parts = split3(jnp.concatenate(pieces, axis=1))
    many = jnp.concatenate(parts, axis=0)

    def products(left, right):
        return lax.dot_general(
            left, right, (((1,), (1,)), ((), ())), preferred_element_type=F32
        )

    first = products(many, parts[0])
    second = products(many[: 2 * count], parts[1])
    third = products(parts[0], parts[2])
    total = (first[:count] + first[count : 2 * count] + first[2 * count :]) + (
        second[:count] + second[count:] + third
    )
    row = lax.broadcasted_iota(jnp.int32, (count, count * count), 0)
    lane = lax.broadcasted_iota(jnp.int32, (count, count * count), 1)
    spread = (lax.rem(lane, count) == row).astype(F32).astype(BF16)
    wide = jnp.dot(
        jnp.concatenate(split3(total), axis=0), spread, preferred_element_type=F32
    )
    wide = wide[:count] + wide[count : 2 * count] + wide[2 * count :]
    flat = jnp.sum(jnp.where(lane // count == row, wide, 0.0), axis=0, keepdims=True)
    half = count * count // 2
    gram[0:1, :] = flat[:, :half]
    gram[1:2, :] = flat[:, half:]


def solve_ones(matrix):
    size = len(matrix)
    lower = [[None] * size for _ in range(size)]
    inverse = [None] * size
    scaled = [[None] * size for _ in range(size)]
    for j in range(size):
        for i in range(j, size):
            value = matrix[i][j]
            for k in range(j):
                value = value - scaled[i][k] * lower[j][k]
            scaled[i][j] = value
        inverse[j] = 1.0 / scaled[j][j]
        for i in range(j + 1, size):
            lower[i][j] = scaled[i][j] * inverse[j]
    forward = []
    for i in range(size):
        value = jnp.ones_like(inverse[0])
        for k in range(i):
            value = value - lower[i][k] * forward[k]
        forward.append(value)
    backward = [None] * size
    for i in reversed(range(size)):
        value = forward[i] * inverse[i]
        for k in range(i + 1, size):
            value = value - lower[k][i] * backward[k]
        backward[i] = value
    total = sum(backward[1:], backward[0])
    return [value / total for value in backward]


def finish_kernel(partials, column, jacobi, shared, shared_last, dipoles, weights):
    core = lax.axis_index("gy")
    slots = column.shape[-1]
    lanes = partials.shape[-1]
    summed = partials[0]
    for k in range(1, partials.shape[0]):
        summed = summed + partials[k]

    def entry(k, j):
        flat = k * 2 * NVEC + j
        row, lane = flat // lanes, flat % lanes
        return jnp.broadcast_to(summed[row : row + 1, lane : lane + 1], (1, lanes))

    first = [[entry(j, k) if j <= k else None for j in range(NVEC)] for k in range(NVEC)]
    early = solve_ones(first)
    mixed = []
    for k in range(1, NVEC):
        value = early[0] * entry(k, NVEC)
        for m in range(1, NVEC):
            value = value + early[m] * entry(k, NVEC + m)
        mixed.append(value)
    square = None
    for m in range(NVEC):
        value = 0.5 * early[m] * entry(NVEC + m, NVEC + m)
        for n in range(m + 1, NVEC):
            value = value + early[n] * entry(NVEC + m, NVEC + n)
        value = early[m] * value
        square = value if square is None else square + value
    second = [
        [first[k][j] if j <= k else None for j in range(1, NVEC)] + [None]
        for k in range(1, NVEC)
    ]
    second.append(mixed + [2.0 * square])
    late = solve_ones(second)

    sub = lax.broadcasted_iota(jnp.int32, (NVEC, lanes), 0)
    lane = lax.broadcasted_iota(jnp.int32, (1, lanes), 1)
    early_column = jnp.zeros((NVEC, lanes), F32)
    late_column = jnp.zeros((NVEC, lanes), F32)
    row = jnp.zeros((1, lanes), F32)
    for k in range(NVEC):
        early_column = jnp.where(sub == k, early[k], early_column)
        if k:
            late_column = jnp.where(sub == k, late[k - 1], late_column)
        row = jnp.where(lane == k, late[k], row)
    weights[...] = row[:, :NVEC]
    reach = slots // lanes
    early_column = jnp.concatenate([early_column] * reach, axis=1)
    late_column = jnp.concatenate([late_column] * reach, axis=1)
    last = jnp.concatenate([late[NVEC - 1]] * reach, axis=1)
    for cell in range(dipoles.shape[1]):
        for i in range(3):
            vectors, field, current, newest, scaled, perm = own_vectors(
                core, cell, i, column, jacobi, shared, shared_last
            )
            induced = jnp.sum(early_column * field, axis=0, keepdims=True)
            output = scaled * (perm + induced)
            kept = jnp.sum(late_column * vectors, axis=0, keepdims=True)
            dipoles[i, cell : cell + 1, :] = kept + last * output


def call(kernel, out_shape, operands, specs=None, scratch=(), megabytes=16, flags=None):
    single = not isinstance(out_shape, (list, tuple))
    outs = [out_shape] if single else list(out_shape)
    result = pl.pallas_call(
        kernel,
        out_shape=outs,
        in_specs=specs or [vmem() for _ in operands],
        out_specs=[vmem() for _ in outs],
        scratch_shapes=list(scratch),
        compiler_params=pltpu.CompilerParams(vmem_limit_bytes=megabytes << 20, flags=flags),
    )(*operands)
    return result[0] if single else result


def shape_of(*dims, dtype=F32):
    return jax.ShapeDtypeStruct(dims, dtype)


def sideways(block):
    count = lax.axis_size(GX)
    cores = lax.axis_size("gy")
    route = []
    for x in range(count):
        for core in range(cores):
            source = (x + 1 - 2 * core) % count
            route.append((source * cores + core, x * cores + core))
    return lax.ppermute(block, GX + ("gy",), route)


def exchanged(block, axes):
    size = lax.axis_size(axes)
    many = jnp.broadcast_to(block[None], (size,) + block.shape)
    return lax.all_to_all(many, axes, 0, 0)


def body(
    positions, polarizability, tile_counts, molecules, perm_field, dipoles, past_out, past_res
):
    own_cells, slots = positions.shape[1], positions.shape[-1]
    cells = 2 * own_cells
    by_comp = [jnp.swapaxes(x[0], 0, 1) for x in (positions, perm_field, dipoles)]
    past_out, past_res = [jnp.moveaxis(x[0], 0, 2) for x in (past_out, past_res)]
    operands = (
        tile_counts[0], by_comp[0], polarizability[0], molecules[0], by_comp[1], by_comp[2], past_out
    )
    packed, groups = call(
        pack_kernel,
        [shape_of(own_cells, ROWS, slots), shape_of(8, slots)],
        [pltpu.with_memory_space_constraint(x, pltpu.HBM) for x in operands],
        [pl.BlockSpec(memory_space=pltpu.HBM)] * 7,
        scratch=[pltpu.SMEM(operands[0].shape, jnp.int32)]
        + [pltpu.VMEM(x.shape, x.dtype) for x in operands[1:]]
        + [pltpu.SemaphoreType.DMA((7,))],
    )
    column = lax.all_gather(packed, "gy").reshape(cells, ROWS, slots)
    beside = sideways(column)
    scratch = [
        pltpu.VMEM((cells, 2 * COMPS * NVEC, slots), BF16),
        pltpu.VMEM((cells, slots, 64), BF16),
        pltpu.VMEM((cells, slots, 64), F32),
    ]

    def pair_shapes(count):
        return [shape_of(count // 2, 4, slots, slots, dtype=BF16)] * 2

    fields_shape = shape_of(cells, 3 * NVEC, slots)
    begun, *own_pairs = call(
        own_pairs_kernel,
        [fields_shape] + pair_shapes(6),
        (column, groups),
        scratch=scratch + [pltpu.VMEM((6, slots, slots), F32)],
    )
    partial, *beside_pairs = call(
        beside_pairs_kernel,
        [fields_shape] + pair_shapes(12),
        (column, beside, begun),
        scratch=scratch + [pltpu.VMEM((12, slots, slots), F32)],
    )
    shared = lax.all_gather(partial, "gy")
    last_shape = shape_of(cells, 3, slots)
    jacobi = call(jacobi_kernel, last_shape, (shared, column))
    jacobi_beside = sideways(jacobi)
    scratch = [pltpu.VMEM((cells, 2 * COMPS, slots), BF16)]
    begun = call(own_apply_kernel, last_shape, (column, jacobi, *own_pairs), scratch=scratch)
    partial = call(
        beside_apply_kernel,
        last_shape,
        (column, beside, jacobi_beside, *beside_pairs, begun),
        scratch=scratch,
    )
    shared_last = lax.all_gather(partial, "gy")
    gram = call(
        gram_kernel,
        shape_of(2, 2 * NVEC * NVEC),
        (column, jacobi, shared, shared_last, past_res),
    )
    gram = jnp.sum(exchanged(gram, ("gx_1", "gy")), axis=0)
    partials = exchanged(gram, ("gx_0",))
    following, weights = call(
        finish_kernel,
        [shape_of(3, own_cells, slots), shape_of(1, NVEC)],
        (partials, column, jacobi, shared, shared_last),
    )
    return (jnp.swapaxes(following, 0, 1)[None], weights.reshape(NVEC))


def solution(mesh):
    torus = Mesh(
        mesh.devices.reshape(mesh.shape["box"], TORUS_Z, TORUS_X, mesh.shape["gy"]),
        ("box", "gx_0", "gx_1", "gy"),
    )
    return jax.shard_map(
        body,
        mesh=torus,
        in_specs=(
            P(BOX_GX, "gy", None, None),
            P(BOX_GX, "gy", None),
            P(BOX_GX, "gy", None),
            P(BOX_GX, "gy", None),
            P(BOX_GX, "gy", None, None),
            P(BOX_GX, "gy", None, None),
            P(BOX_GX, "gy", None, None, None),
            P(BOX_GX, "gy", None, None, None),
        ),
        out_specs=(P(BOX_GX, "gy", None, None), P("box")),
        check_vma=False,
    )
```

```python
import functools

import jax
import jax.numpy as jnp
from jax import lax
from jax.experimental import pallas as pl
from jax.experimental.pallas import tpu as pltpu
from jax.sharding import Mesh
from jax.sharding import PartitionSpec as P

GX = ("gx_0", "gx_1")
BOX_GX = ("box", "gx_0", "gx_1")
TORUS_Z = 16
TORUS_X = 8

CELL_SIDE = 9.0
CUTOFF_SQ = 81.0
SOFTENING = 0.25
THOLE_DAMP = 0.39
LN2 = 0.6931471805599453

NVEC = 8
ROW_XYZ = 24
ROW_POLAR = 27
ROW_OCC = 28
ROW_PERM = 29
ROWS = 32
COMPS = 16
CHUNK = 16
F32 = jnp.float32
BF16 = jnp.bfloat16


def vmem():
    return pl.BlockSpec(memory_space=pltpu.VMEM)


def smem():
    return pl.BlockSpec(memory_space=pltpu.SMEM)


def split3(value):
    first = value.astype(BF16)
    rest = value - first.astype(F32)
    second = rest.astype(BF16)
    third = (rest - second.astype(F32)).astype(BF16)
    return first, second, third


def split2(value):
    first = value.astype(BF16)
    return first, (value - first.astype(F32)).astype(BF16)


def pack_kernel(*refs):
    sources, packed, groups = refs[:7], refs[7], refs[8]
    held, semaphores = refs[9:16], refs[16]
    copies = [
        pltpu.make_async_copy(source, target, semaphores.at[at])
        for at, (source, target) in enumerate(zip(sources, held))
    ]
    for copy in copies:
        copy.start()
    for copy in copies:
        copy.wait()
    counts, positions, polarity, molecules, permanent, dipoles, past_out = held
    cells, slots = polarity.shape
    tiles = sources[0].shape[1]
    tile = slots // tiles
    slot = lax.broadcasted_iota(jnp.int32, (1, slots), 1)
    groups[...] = jnp.zeros(groups.shape, F32)
    for cell in range(cells):
        occ = (slot < counts[cell, 0]).astype(F32)
        for t in range(1, tiles):
            inside = (slot - t * tile < counts[cell, t]).astype(F32)
            occ = jnp.where(slot >= t * tile, inside, occ)
        at = slice(cell, cell + 1)
        for comp in range(3):
            for k in range(NVEC - 1):
                row = comp * NVEC + k
                packed[cell, row : row + 1, :] = past_out[k, comp, at, :] * occ
            row = comp * NVEC + NVEC - 1
            packed[cell, row : row + 1, :] = dipoles[comp, at, :] * occ
            centre = 0.5 * CELL_SIDE if comp < 2 else CELL_SIDE
            row = (positions[comp, at, :] - centre) * (1.0 / CELL_SIDE)
            packed[cell, ROW_XYZ + comp : ROW_XYZ + comp + 1, :] = row
            packed[cell, ROW_PERM + comp : ROW_PERM + comp + 1, :] = permanent[comp, at, :]
        packed[cell, ROW_POLAR : ROW_POLAR + 1, :] = polarity[at, :]
        packed[cell, ROW_OCC : ROW_OCC + 1, :] = occ
        groups[at, :] = molecules[at, :].astype(F32)


def source_moments(coords, vectors):
    vx, vy, vz = [v * (1.0 / CELL_SIDE**3) for v in vectors]
    dot = coords[0] * vx + coords[1] * vy + coords[2] * vz
    comps = [coords[i] * dot for i in range(3)]
    comps += [coords[i] * v for i in range(3) for v in (vx, vy, vz)]
    return comps + [dot, vx, vy, vz]


def fields_of(moments, isotropic, target):
    along = target[0] * moments[13] + target[1] * moments[14] + target[2] * moments[15]
    shared = moments[12] - along
    out = []
    for i in range(3):
        part = moments[i] - target[i] * shared
        for j in range(3):
            part = part - target[j] * moments[3 + 3 * i + j]
        out.append(3.0 * part - isotropic[i])
    return out


def beside_row(at, core, cells):
    half = cells // 2
    return (core if at < half else 1 - core) * half + at % half


def beside_block(index, core, cells):
    source, step = index // 3, index % 3 - 1
    target = lax.rem(beside_row(source, core, cells) - step + cells, cells)
    return source, target, 0, (1 - 2 * core).astype(F32), step, False


def column_block(index, core, cells):
    own_at, step = index // 3, index % 3 - 1
    target = 2 * core + own_at
    return lax.rem(target + step + cells, cells), target, own_at, 0.0, step, step == 0


def place_of(column, block):
    _, target, _, move_x, step, _ = block
    x = column[target, ROW_XYZ : ROW_XYZ + 1, :] - move_x
    y = column[target, ROW_XYZ + 1 : ROW_XYZ + 2, :] - float(step)
    return x, y, column[target, ROW_XYZ + 2 : ROW_XYZ + 3, :]


def filled_rows(rows, count):
    slots = rows[0].shape[-1]
    return jnp.concatenate(rows + [jnp.zeros((count - len(rows), slots), F32)], axis=0)


def paired_parts(value, order):
    parts = [part.astype(F32) for part in split3(value)]
    blank = jnp.zeros_like(value)
    return [parts[at] for at in order] + [blank]


def pair_loop(count, block_at, column, groups, fields, even, odd, moments, feats, columns, square):
    cells, slots = column.shape[0], column.shape[-1]
    core = lax.axis_index("gy")

    def info(index):
        return block_at(index, core, cells)

    def distances(index):
        block = info(index)
        x, y, z = place_of(column, block)
        norm = x * x + y * y + z * z
        rows = filled_rows([-2.0 * x, -2.0 * y, -2.0 * z, norm, jnp.ones_like(norm)], 8)
        rhs = jnp.concatenate(
            [jnp.zeros_like(rows)] + paired_parts(rows, (0, 0, 0, 1, 1, 2)), axis=0
        ).astype(BF16)
        square[index] = jnp.dot(feats[block[0]], rhs, preferred_element_type=F32)

    def produce(index, out, at):
        block = info(index)
        source, target, own_at = block[:3]
        scale = lax.rsqrt(column[target, ROW_POLAR : ROW_POLAR + 1, :])
        scale = scale * (-THOLE_DAMP * CELL_SIDE**3 / LN2)
        if block[5]:
            group = groups[own_at : own_at + 1, :]
        for chunk in range(slots // CHUNK):
            part = slice(chunk * CHUNK, (chunk + 1) * CHUNK)
            near = columns[source, part, :]
            squared = square[index, part, :]
            inverse = lax.rsqrt(squared)
            inverse_sq = inverse * inverse
            exponent = (squared * squared * inverse) * (near[:, 0:1] * scale)
            damping = jnp.exp2(exponent)
            taper = jnp.maximum(1.0 - squared, 0.0)
            weight = (taper * taper) * (inverse_sq * inverse)
            if block[5]:
                weight = jnp.where(near[:, 1:2] == group, 0.0, weight)
            undamped = 1.0 - damping
            isotropic = weight * undamped
            tensorial = (weight * inverse_sq) * (undamped + (LN2 * exponent) * damping)
            for k, value in enumerate(split2(tensorial) + split2(isotropic)):
                out[at, k, part, :] = value

    def apply(index, pairs, at):
        block = info(index)
        lhs = moments[block[0]]
        size = COMPS * NVEC
        low, band = size - 4 * NVEC, 4 * NVEC
        first = jnp.dot(lhs, pairs[at, 0], preferred_element_type=F32)
        second = jnp.dot(lhs[:size], pairs[at, 1], preferred_element_type=F32)
        total = first[:size] + first[size:] + second
        iso_lhs = jnp.concatenate([lhs[low:size], lhs[size + low :]], 0)
        first = jnp.dot(iso_lhs, pairs[at, 2], preferred_element_type=F32)
        second = jnp.dot(lhs[low:size], pairs[at, 3], preferred_element_type=F32)
        iso = first[:band] + first[band:] + second
        result = fields_of(
            [total[NVEC * i : NVEC * i + NVEC] for i in range(COMPS)],
            [iso[NVEC * i : NVEC * i + NVEC] for i in range(1, 4)],
            place_of(column, block),
        )
        for i in range(3):
            fields[block[1], NVEC * i : NVEC * i + NVEC, :] += result[i]

    ahead = 2
    for index in range(count + 1):
        for later in range(ahead + 1) if index == 0 else (index + ahead,):
            if later < count:
                distances(later)
        if index < count:
            produce(index, (even, odd)[index % 2], index // 2)
        if index:
            last = index - 1
            apply(last, (even, odd)[last % 2], last // 2)


def load_sources(cells, groups, moments, feats, columns):
    core = lax.axis_index("gy")
    for at, cell in enumerate(cells):
        coords = [cell[ROW_XYZ + i : ROW_XYZ + i + 1] for i in range(3)]
        vectors = [cell[NVEC * i : NVEC * i + NVEC] for i in range(3)]
        stacked = jnp.concatenate(source_moments(coords, vectors), axis=0)
        for part, value in enumerate(split2(stacked)):
            moments[at, part * COMPS * NVEC : (part + 1) * COMPS * NVEC, :] = value
        norm = coords[0] * coords[0] + coords[1] * coords[1] + coords[2] * coords[2]
        norm = norm + SOFTENING / CELL_SIDE**2
        head = [lax.rsqrt(cell[ROW_POLAR : ROW_POLAR + 1])]
        if groups is not None:
            own = jnp.clip(at - 2 * core, 0, 1)
            head.append(groups[pl.ds(own, 1), :])
        rows = filled_rows(coords + [jnp.ones_like(norm), norm], 8)
        tall = jnp.concatenate(
            [filled_rows(head, 8)] + paired_parts(rows, (0, 1, 2, 0, 1, 0)), axis=0
        ).T
        columns[at] = tall
        feats[at] = tall.astype(BF16)


def own_pairs_kernel(column, groups, fields, even, odd, moments, feats, columns, square):
    fields[...] = jnp.zeros(fields.shape, F32)
    load_sources([column[at] for at in range(column.shape[0])], groups, moments, feats, columns)
    pair_loop(6, column_block, column, groups, fields, even, odd, moments, feats, columns, square)


def beside_pairs_kernel(
    column, straight, crossed, begun, fields, newest, even, odd, moments, feats, columns, square
):
    fields[...] = begun[...]
    cells = [ref[at] for ref in (straight, crossed) for at in range(ref.shape[0])]
    load_sources(cells, None, moments, feats, columns)
    pair_loop(12, beside_block, column, None, fields, even, odd, moments, feats, columns, square)
    for cell in range(newest.shape[0]):
        for i in range(3):
            row = NVEC * i + NVEC - 1
            newest[cell, i : i + 1, :] = fields[cell, row : row + 1, :]


def jacobi_of(cell, fields):
    scaled = cell[ROW_POLAR : ROW_POLAR + 1] * cell[ROW_OCC : ROW_OCC + 1]
    return [scaled * (cell[ROW_PERM + i : ROW_PERM + i + 1] + fields[i]) for i in range(3)]


def apply_pairs(count, block_at, column, cells, vectors, even, odd, fields, moments):
    core = lax.axis_index("gy")
    for at, (cell, values) in enumerate(zip(cells, vectors)):
        coords = [cell[ROW_XYZ + i : ROW_XYZ + i + 1] for i in range(3)]
        stacked = jnp.concatenate(source_moments(coords, values), axis=0)
        for part, value in enumerate(split2(stacked)):
            moments[at, part * COMPS : (part + 1) * COMPS, :] = value
    for index in range(count):
        block = block_at(index, core, len(cells))
        pairs, at = (even, odd)[index % 2], index // 2
        lhs = moments[block[0]]
        first = jnp.dot(lhs, pairs[at, 0], preferred_element_type=F32)
        second = jnp.dot(lhs[:COMPS], pairs[at, 1], preferred_element_type=F32)
        total = first[:COMPS] + first[COMPS:] + second
        first = jnp.dot(lhs, pairs[at, 2], preferred_element_type=F32)
        second = jnp.dot(lhs[:COMPS], pairs[at, 3], preferred_element_type=F32)
        iso = first[:COMPS] + first[COMPS:] + second
        result = fields_of(
            [total[i : i + 1] for i in range(COMPS)],
            [iso[i : i + 1] for i in range(COMPS - 3, COMPS)],
            place_of(column, block),
        )
        for i in range(3):
            fields[block[1], i : i + 1, :] += result[i]


def own_apply_kernel(column, shared, even, odd, jacobi, fields, moments):
    fields[...] = jnp.zeros(fields.shape, F32)
    cells = [column[at] for at in range(column.shape[0])]
    vectors = []
    for at, cell in enumerate(cells):
        rows = [slice(NVEC * i + NVEC - 1, NVEC * i + NVEC) for i in range(3)]
        summed = [shared[0, at, row, :] + shared[1, at, row, :] for row in rows]
        vectors.append(jacobi_of(cell, summed))
        for i in range(3):
            jacobi[at, i : i + 1, :] = vectors[at][i]
    apply_pairs(6, column_block, column, cells, vectors, even, odd, fields, moments)


def beside_apply_kernel(
    column, straight, crossed, newest, newest_crossed, even, odd, begun, fields, moments
):
    core = lax.axis_index("gy")
    fields[...] = begun[...]
    cells = [ref[at] for ref in (straight, crossed) for at in range(ref.shape[0])]
    vectors = []
    for at, cell in enumerate(cells):
        y = beside_row(at, core, len(cells))
        summed = newest[y] + newest_crossed[y]
        vectors.append(jacobi_of(cell, [summed[i : i + 1] for i in range(3)]))
    apply_pairs(12, beside_block, column, cells, vectors, even, odd, fields, moments)


def own_vectors(core, cell, i, column, jacobi, shared, shared_last):
    at = 2 * core + cell
    slots = column.shape[-1]
    last = lax.broadcasted_iota(jnp.int32, (NVEC, slots), 0) == NVEC - 1
    rows = slice(NVEC * i, NVEC * i + NVEC)
    vectors = column[at, rows, :]
    current = vectors[NVEC - 1 :]
    jacobi_row = jacobi[at, i : i + 1, :]
    vectors = jnp.where(last, jacobi_row, vectors)
    field = shared[0, at, rows, :] + shared[1, at, rows, :]
    newest = shared_last[0, at, i : i + 1, :] + shared_last[1, at, i : i + 1, :]
    field = jnp.where(last, newest, field)
    scaled = column[at, ROW_POLAR : ROW_POLAR + 1, :] * column[at, ROW_OCC : ROW_OCC + 1, :]
    perm = column[at, ROW_PERM + i : ROW_PERM + i + 1, :]
    return vectors, field, current, jacobi_row, scaled, perm


def gram_kernel(column, jacobi, shared, shared_last, past_res, gram):
    core = lax.axis_index("gy")
    pieces = []
    for cell in range(past_res.shape[2]):
        occ = column[2 * core + cell, ROW_OCC : ROW_OCC + 1, :]
        for i in range(3):
            vectors, field, current, newest, scaled, perm = own_vectors(
                core, cell, i, column, jacobi, shared, shared_last
            )
            old = [past_res[k, i, cell : cell + 1, :] for k in range(NVEC - 1)]
            residual = jnp.concatenate(old + [newest - current], axis=0) * occ
            implied = scaled * (perm + field) - vectors
            pieces.append(jnp.concatenate([residual, implied], axis=0))
    count = 2 * NVEC
    parts = split3(jnp.concatenate(pieces, axis=1))
    many = jnp.concatenate(parts, axis=0)

    def products(left, right):
        return lax.dot_general(
            left, right, (((1,), (1,)), ((), ())), preferred_element_type=F32
        )

    first = products(many, parts[0])
    second = products(many[: 2 * count], parts[1])
    third = products(parts[0], parts[2])
    total = (first[:count] + first[count : 2 * count] + first[2 * count :]) + (
        second[:count] + second[count:] + third
    )
    row = lax.broadcasted_iota(jnp.int32, (count, count * count), 0)
    lane = lax.broadcasted_iota(jnp.int32, (count, count * count), 1)
    spread = (lax.rem(lane, count) == row).astype(F32).astype(BF16)
    wide = jnp.dot(
        jnp.concatenate(split3(total), axis=0), spread, preferred_element_type=F32
    )
    wide = wide[:count] + wide[count : 2 * count] + wide[2 * count :]
    flat = jnp.sum(jnp.where(lane // count == row, wide, 0.0), axis=0, keepdims=True)
    half = count * count // 2
    gram[0:1, :] = flat[:, :half]
    gram[1:2, :] = flat[:, half:]


def solve_ones(matrix):
    size = len(matrix)
    lower = [[None] * size for _ in range(size)]
    inverse = [None] * size
    scaled = [[None] * size for _ in range(size)]
    for j in range(size):
        for i in range(j, size):
            value = matrix[i][j]
            for k in range(j):
                value = value - scaled[i][k] * lower[j][k]
            scaled[i][j] = value
        inverse[j] = 1.0 / scaled[j][j]
        for i in range(j + 1, size):
            lower[i][j] = scaled[i][j] * inverse[j]
    forward = []
    for i in range(size):
        value = jnp.ones_like(inverse[0])
        for k in range(i):
            value = value - lower[i][k] * forward[k]
        forward.append(value)
    backward = [None] * size
    for i in reversed(range(size)):
        value = forward[i] * inverse[i]
        for k in range(i + 1, size):
            value = value - lower[k][i] * backward[k]
        backward[i] = value
    total = sum(backward[1:], backward[0])
    return [value / total for value in backward]


def finish_kernel(partials, column, jacobi, shared, shared_last, dipoles, weights):
    core = lax.axis_index("gy")
    slots = column.shape[-1]
    lanes = partials.shape[-1]
    summed = partials[0]
    for k in range(1, partials.shape[0]):
        summed = summed + partials[k]

    def entry(k, j):
        flat = k * 2 * NVEC + j
        row, lane = flat // lanes, flat % lanes
        return jnp.broadcast_to(summed[row : row + 1, lane : lane + 1], (1, lanes))

    first = [[entry(j, k) if j <= k else None for j in range(NVEC)] for k in range(NVEC)]
    early = solve_ones(first)
    mixed = []
    for k in range(1, NVEC):
        value = early[0] * entry(k, NVEC)
        for m in range(1, NVEC):
            value = value + early[m] * entry(k, NVEC + m)
        mixed.append(value)
    square = None
    for m in range(NVEC):
        value = 0.5 * early[m] * entry(NVEC + m, NVEC + m)
        for n in range(m + 1, NVEC):
            value = value + early[n] * entry(NVEC + m, NVEC + n)
        value = early[m] * value
        square = value if square is None else square + value
    second = [
        [first[k][j] if j <= k else None for j in range(1, NVEC)] + [None]
        for k in range(1, NVEC)
    ]
    second.append(mixed + [2.0 * square])
    late = solve_ones(second)

    sub = lax.broadcasted_iota(jnp.int32, (NVEC, lanes), 0)
    lane = lax.broadcasted_iota(jnp.int32, (1, lanes), 1)
    early_column = jnp.zeros((NVEC, lanes), F32)
    late_column = jnp.zeros((NVEC, lanes), F32)
    row = jnp.zeros((1, lanes), F32)
    for k in range(NVEC):
        early_column = jnp.where(sub == k, early[k], early_column)
        if k:
            late_column = jnp.where(sub == k, late[k - 1], late_column)
        row = jnp.where(lane == k, late[k], row)
    weights[...] = row[:, :NVEC]
    reach = slots // lanes
    early_column = jnp.concatenate([early_column] * reach, axis=1)
    late_column = jnp.concatenate([late_column] * reach, axis=1)
    last = jnp.concatenate([late[NVEC - 1]] * reach, axis=1)
    for cell in range(dipoles.shape[1]):
        for i in range(3):
            vectors, field, current, newest, scaled, perm = own_vectors(
                core, cell, i, column, jacobi, shared, shared_last
            )
            induced = jnp.sum(early_column * field, axis=0, keepdims=True)
            output = scaled * (perm + induced)
            kept = jnp.sum(late_column * vectors, axis=0, keepdims=True)
            dipoles[i, cell : cell + 1, :] = kept + last * output


def call(kernel, out_shape, operands, specs=None, scratch=(), megabytes=16, flags=None):
    single = not isinstance(out_shape, (list, tuple))
    outs = [out_shape] if single else list(out_shape)
    result = pl.pallas_call(
        kernel,
        out_shape=outs,
        in_specs=specs or [vmem() for _ in operands],
        out_specs=[vmem() for _ in outs],
        scratch_shapes=list(scratch),
        compiler_params=pltpu.CompilerParams(vmem_limit_bytes=megabytes << 20, flags=flags),
    )(*operands)
    return result[0] if single else result


def shape_of(*dims, dtype=F32):
    return jax.ShapeDtypeStruct(dims, dtype)


def sideways(block):
    count = lax.axis_size(GX)
    cores = lax.axis_size("gy")
    received = []
    for other in (0, 1):
        route = []
        for x in range(count):
            for core in range(cores):
                source = (x + 1 - 2 * core) % count
                route.append((source * cores + (core + other) % cores, x * cores + core))
        received.append(lax.ppermute(block, GX + ("gy",), route))
    return received


def exchanged(block, axes):
    size = lax.axis_size(axes)
    many = jnp.broadcast_to(block[None], (size,) + block.shape)
    return lax.all_to_all(many, axes, 0, 0)


def body(
    positions, polarizability, tile_counts, molecules, perm_field, dipoles, past_out, past_res
):
    own_cells, slots = positions.shape[1], positions.shape[-1]
    cells = 2 * own_cells
    by_comp = [jnp.swapaxes(x[0], 0, 1) for x in (positions, perm_field, dipoles)]
    past_out, past_res = [jnp.moveaxis(x[0], 0, 2) for x in (past_out, past_res)]
    operands = (
        tile_counts[0], by_comp[0], polarizability[0], molecules[0], by_comp[1], by_comp[2], past_out
    )
    packed, groups = call(
        pack_kernel,
        [shape_of(own_cells, ROWS, slots), shape_of(8, slots)],
        [pltpu.with_memory_space_constraint(x, pltpu.HBM) for x in operands],
        [pl.BlockSpec(memory_space=pltpu.HBM)] * 7,
        scratch=[pltpu.SMEM(operands[0].shape, jnp.int32)]
        + [pltpu.VMEM(x.shape, x.dtype) for x in operands[1:]]
        + [pltpu.SemaphoreType.DMA((7,))],
    )
    straight, crossed = sideways(packed)
    column = lax.all_gather(packed, "gy").reshape(cells, ROWS, slots)
    scratch = [
        pltpu.VMEM((cells, 2 * COMPS * NVEC, slots), BF16),
        pltpu.VMEM((cells, slots, 64), BF16),
        pltpu.VMEM((cells, slots, 64), F32),
    ]

    def pair_shapes(count):
        return [shape_of(count // 2, 4, slots, slots, dtype=BF16)] * 2

    fields_shape = shape_of(cells, 3 * NVEC, slots)
    begun, *own_pairs = call(
        own_pairs_kernel,
        [fields_shape] + pair_shapes(6),
        (column, groups),
        scratch=scratch + [pltpu.VMEM((6, slots, slots), F32)],
    )
    last_shape = shape_of(cells, 3, slots)
    partial, newest, *beside_pairs = call(
        beside_pairs_kernel,
        [fields_shape, last_shape] + pair_shapes(12),
        (column, straight, crossed, begun),
        scratch=scratch + [pltpu.VMEM((12, slots, slots), F32)],
    )
    newest, newest_crossed = sideways(newest)
    shared = lax.all_gather(partial, "gy")
    scratch = [pltpu.VMEM((cells, 2 * COMPS, slots), BF16)]
    jacobi, begun = call(
        own_apply_kernel, [last_shape, last_shape], (column, shared, *own_pairs), scratch=scratch
    )
    partial = call(
        beside_apply_kernel,
        last_shape,
        (column, straight, crossed, newest, newest_crossed, *beside_pairs, begun),
        scratch=scratch,
    )
    shared_last = lax.all_gather(partial, "gy")
    gram = call(
        gram_kernel,
        shape_of(2, 2 * NVEC * NVEC),
        (column, jacobi, shared, shared_last, past_res),
    )
    gram = jnp.sum(exchanged(gram, ("gx_1", "gy")), axis=0)
    partials = exchanged(gram, ("gx_0",))
    following, weights = call(
        finish_kernel,
        [shape_of(3, own_cells, slots), shape_of(1, NVEC)],
        (partials, column, jacobi, shared, shared_last),
    )
    return (jnp.swapaxes(following, 0, 1)[None], weights.reshape(NVEC))


def solution(mesh):
    torus = Mesh(
        mesh.devices.reshape(mesh.shape["box"], TORUS_Z, TORUS_X, mesh.shape["gy"]),
        ("box", "gx_0", "gx_1", "gy"),
    )
    return jax.shard_map(
        body,
        mesh=torus,
        in_specs=(
            P(BOX_GX, "gy", None, None),
            P(BOX_GX, "gy", None),
            P(BOX_GX, "gy", None),
            P(BOX_GX, "gy", None),
            P(BOX_GX, "gy", None, None),
            P(BOX_GX, "gy", None, None),
            P(BOX_GX, "gy", None, None, None),
            P(BOX_GX, "gy", None, None, None),
        ),
        out_specs=(P(BOX_GX, "gy", None, None), P("box")),
        check_vma=False,
    )
```

```python
import functools

import jax
import jax.numpy as jnp
from jax import lax
from jax.experimental import pallas as pl
from jax.experimental.pallas import tpu as pltpu
from jax.sharding import Mesh
from jax.sharding import PartitionSpec as P

GX = ("gx_0", "gx_1")
BOX_GX = ("box", "gx_0", "gx_1")
TORUS_Z = 16
TORUS_X = 8

CELL_SIDE = 9.0
CUTOFF_SQ = 81.0
SOFTENING = 0.25
THOLE_DAMP = 0.39
LN2 = 0.6931471805599453

NVEC = 8
ROW_XYZ = 24
ROW_POLAR = 27
ROW_OCC = 28
ROW_PERM = 29
ROWS = 32
COMPS = 16
CHUNK = 16
F32 = jnp.float32
BF16 = jnp.bfloat16


def vmem():
    return pl.BlockSpec(memory_space=pltpu.VMEM)


def smem():
    return pl.BlockSpec(memory_space=pltpu.SMEM)


def split3(value):
    first = value.astype(BF16)
    rest = value - first.astype(F32)
    second = rest.astype(BF16)
    third = (rest - second.astype(F32)).astype(BF16)
    return first, second, third


def split2(value):
    first = value.astype(BF16)
    return first, (value - first.astype(F32)).astype(BF16)


def pack_kernel(*refs):
    sources, packed, groups = refs[:7], refs[7], refs[8]
    held, semaphores = refs[9:16], refs[16]
    copies = [
        pltpu.make_async_copy(source, target, semaphores.at[at])
        for at, (source, target) in enumerate(zip(sources, held))
    ]
    for copy in copies:
        copy.start()
    for copy in copies:
        copy.wait()
    counts, positions, polarity, molecules, permanent, dipoles, past_out = held
    cells, slots = polarity.shape
    tiles = sources[0].shape[1]
    tile = slots // tiles
    slot = lax.broadcasted_iota(jnp.int32, (1, slots), 1)
    groups[...] = jnp.zeros(groups.shape, F32)
    for cell in range(cells):
        occ = (slot < counts[cell, 0]).astype(F32)
        for t in range(1, tiles):
            inside = (slot - t * tile < counts[cell, t]).astype(F32)
            occ = jnp.where(slot >= t * tile, inside, occ)
        at = slice(cell, cell + 1)
        for comp in range(3):
            for k in range(NVEC - 1):
                row = comp * NVEC + k
                packed[cell, row : row + 1, :] = past_out[k, comp, at, :] * occ
            row = comp * NVEC + NVEC - 1
            packed[cell, row : row + 1, :] = dipoles[comp, at, :] * occ
            centre = 0.5 * CELL_SIDE if comp < 2 else CELL_SIDE
            row = (positions[comp, at, :] - centre) * (1.0 / CELL_SIDE)
            packed[cell, ROW_XYZ + comp : ROW_XYZ + comp + 1, :] = row
            packed[cell, ROW_PERM + comp : ROW_PERM + comp + 1, :] = permanent[comp, at, :]
        packed[cell, ROW_POLAR : ROW_POLAR + 1, :] = polarity[at, :]
        packed[cell, ROW_OCC : ROW_OCC + 1, :] = occ
        groups[at, :] = molecules[at, :].astype(F32)


def source_moments(coords, vectors):
    vx, vy, vz = [v * (1.0 / CELL_SIDE**3) for v in vectors]
    dot = coords[0] * vx + coords[1] * vy + coords[2] * vz
    comps = [coords[i] * dot for i in range(3)]
    comps += [coords[i] * v for i in range(3) for v in (vx, vy, vz)]
    return comps + [dot, vx, vy, vz]


def fields_of(moments, isotropic, target):
    along = target[0] * moments[13] + target[1] * moments[14] + target[2] * moments[15]
    shared = moments[12] - along
    out = []
    for i in range(3):
        part = moments[i] - target[i] * shared
        for j in range(3):
            part = part - target[j] * moments[3 + 3 * i + j]
        out.append(3.0 * part - isotropic[i])
    return out


def beside_row(at, core, cells):
    half = cells // 2
    return (core if at < half else 1 - core) * half + at % half


def beside_block(index, core, cells):
    source, step = index // 3, index % 3 - 1
    target = lax.rem(beside_row(source, core, cells) - step + cells, cells)
    return source, target, 0, (2 * core - 1).astype(F32), step, False


def column_block(index, core, cells):
    own_at, step = index // 3, index % 3 - 1
    target = 2 * core + own_at
    return lax.rem(target + step + cells, cells), target, own_at, 0.0, step, step == 0


def place_of(column, block):
    _, target, _, move_x, step, _ = block
    x = column[target, ROW_XYZ : ROW_XYZ + 1, :] - move_x
    y = column[target, ROW_XYZ + 1 : ROW_XYZ + 2, :] - float(step)
    return x, y, column[target, ROW_XYZ + 2 : ROW_XYZ + 3, :]


def filled_rows(rows, count):
    slots = rows[0].shape[-1]
    return jnp.concatenate(rows + [jnp.zeros((count - len(rows), slots), F32)], axis=0)


def paired_parts(value, order):
    parts = [part.astype(F32) for part in split3(value)]
    blank = jnp.zeros_like(value)
    return [parts[at] for at in order] + [blank]


def pair_loop(count, block_at, column, groups, fields, even, odd, moments, feats, columns, square):
    cells, slots = column.shape[0], column.shape[-1]
    core = lax.axis_index("gy")

    def info(index):
        return block_at(index, core, cells)

    def distances(index):
        block = info(index)
        x, y, z = place_of(column, block)
        norm = x * x + y * y + z * z
        rows = filled_rows([-2.0 * x, -2.0 * y, -2.0 * z, norm, jnp.ones_like(norm)], 8)
        rhs = jnp.concatenate(
            [jnp.zeros_like(rows)] + paired_parts(rows, (0, 0, 0, 1, 1, 2)), axis=0
        ).astype(BF16)
        square[index] = jnp.dot(feats[block[0]], rhs, preferred_element_type=F32)

    def produce(index, out, at):
        block = info(index)
        source, target, own_at = block[:3]
        scale = lax.rsqrt(column[target, ROW_POLAR : ROW_POLAR + 1, :])
        scale = scale * (-THOLE_DAMP * CELL_SIDE**3 / LN2)
        if block[5]:
            group = groups[own_at : own_at + 1, :]
        for chunk in range(slots // CHUNK):
            part = slice(chunk * CHUNK, (chunk + 1) * CHUNK)
            near = columns[source, part, :]
            squared = square[index, part, :]
            inverse = lax.rsqrt(squared)
            inverse_sq = inverse * inverse
            exponent = (squared * squared * inverse) * (near[:, 0:1] * scale)
            damping = jnp.exp2(exponent)
            taper = jnp.maximum(1.0 - squared, 0.0)
            weight = (taper * taper) * (inverse_sq * inverse)
            if block[5]:
                weight = jnp.where(near[:, 1:2] == group, 0.0, weight)
            undamped = 1.0 - damping
            isotropic = weight * undamped
            tensorial = (weight * inverse_sq) * (undamped + (LN2 * exponent) * damping)
            for k, value in ((0, tensorial), (2, isotropic)):
                out[at, k, part, :] = value.astype(BF16)
                rest = value - out[at, k, part, :].astype(F32)
                out[at, k + 1, part, :] = rest.astype(BF16)

    def apply(index, pairs, at):
        block = info(index)
        lhs = moments[block[0]]
        size = COMPS * NVEC
        low, band = size - 4 * NVEC, 4 * NVEC
        first = jnp.dot(lhs, pairs[at, 0], preferred_element_type=F32)
        second = jnp.dot(lhs[:size], pairs[at, 1], preferred_element_type=F32)
        total = first[:size] + first[size:] + second
        iso_lhs = jnp.concatenate([lhs[low:size], lhs[size + low :]], 0)
        first = jnp.dot(iso_lhs, pairs[at, 2], preferred_element_type=F32)
        second = jnp.dot(lhs[low:size], pairs[at, 3], preferred_element_type=F32)
        iso = first[:band] + first[band:] + second
        result = fields_of(
            [total[NVEC * i : NVEC * i + NVEC] for i in range(COMPS)],
            [iso[NVEC * i : NVEC * i + NVEC] for i in range(1, 4)],
            place_of(column, block),
        )
        for i in range(3):
            fields[block[1], NVEC * i : NVEC * i + NVEC, :] += result[i]

    ahead = 2
    for index in range(count + 1):
        for later in range(ahead + 1) if index == 0 else (index + ahead,):
            if later < count:
                distances(later)
        if index < count:
            produce(index, (even, odd)[index % 2], index // 2)
        if index:
            last = index - 1
            apply(last, (even, odd)[last % 2], last // 2)


def load_sources(cells, groups, moments, feats, columns):
    core = lax.axis_index("gy")
    for at, cell in enumerate(cells):
        coords = [cell[ROW_XYZ + i : ROW_XYZ + i + 1] for i in range(3)]
        vectors = [cell[NVEC * i : NVEC * i + NVEC] for i in range(3)]
        stacked = jnp.concatenate(source_moments(coords, vectors), axis=0)
        for part, value in enumerate(split2(stacked)):
            moments[at, part * COMPS * NVEC : (part + 1) * COMPS * NVEC, :] = value
        norm = coords[0] * coords[0] + coords[1] * coords[1] + coords[2] * coords[2]
        norm = norm + SOFTENING / CELL_SIDE**2
        head = [lax.rsqrt(cell[ROW_POLAR : ROW_POLAR + 1])]
        if groups is not None:
            own = jnp.clip(at - 2 * core, 0, 1)
            head.append(groups[pl.ds(own, 1), :])
        rows = filled_rows(coords + [jnp.ones_like(norm), norm], 8)
        tall = jnp.concatenate(
            [filled_rows(head, 8)] + paired_parts(rows, (0, 1, 2, 0, 1, 0)), axis=0
        ).T
        columns[at] = tall
        feats[at] = tall.astype(BF16)


def own_pairs_kernel(column, groups, fields, even, odd, moments, feats, columns, square):
    fields[...] = jnp.zeros(fields.shape, F32)
    load_sources([column[at] for at in range(column.shape[0])], groups, moments, feats, columns)
    pair_loop(6, column_block, column, groups, fields, even, odd, moments, feats, columns, square)


def beside_pairs_kernel(
    column, straight, crossed, begun, fields, newest, even, odd, moments, feats, columns, square
):
    fields[...] = begun[...]
    cells = [ref[at] for ref in (straight, crossed) for at in range(ref.shape[0])]
    load_sources(cells, None, moments, feats, columns)
    pair_loop(12, beside_block, column, None, fields, even, odd, moments, feats, columns, square)
    for cell in range(newest.shape[0]):
        for i in range(3):
            row = NVEC * i + NVEC - 1
            newest[cell, i : i + 1, :] = fields[cell, row : row + 1, :]


def jacobi_of(cell, fields):
    scaled = cell[ROW_POLAR : ROW_POLAR + 1] * cell[ROW_OCC : ROW_OCC + 1]
    return [scaled * (cell[ROW_PERM + i : ROW_PERM + i + 1] + fields[i]) for i in range(3)]


def apply_pairs(count, block_at, column, cells, vectors, even, odd, fields, moments):
    core = lax.axis_index("gy")
    for at, (cell, values) in enumerate(zip(cells, vectors)):
        coords = [cell[ROW_XYZ + i : ROW_XYZ + i + 1] for i in range(3)]
        stacked = jnp.concatenate(source_moments(coords, values), axis=0)
        for part, value in enumerate(split2(stacked)):
            moments[at, part * COMPS : (part + 1) * COMPS, :] = value
    for index in range(count):
        block = block_at(index, core, len(cells))
        pairs, at = (even, odd)[index % 2], index // 2
        lhs = moments[block[0]]
        first = jnp.dot(lhs, pairs[at, 0], preferred_element_type=F32)
        second = jnp.dot(lhs[:COMPS], pairs[at, 1], preferred_element_type=F32)
        total = first[:COMPS] + first[COMPS:] + second
        first = jnp.dot(lhs, pairs[at, 2], preferred_element_type=F32)
        second = jnp.dot(lhs[:COMPS], pairs[at, 3], preferred_element_type=F32)
        iso = first[:COMPS] + first[COMPS:] + second
        result = fields_of(
            [total[i : i + 1] for i in range(COMPS)],
            [iso[i : i + 1] for i in range(COMPS - 3, COMPS)],
            place_of(column, block),
        )
        for i in range(3):
            fields[block[1], i : i + 1, :] += result[i]


def own_apply_kernel(column, shared, even, odd, jacobi, fields, moments):
    fields[...] = jnp.zeros(fields.shape, F32)
    cells = [column[at] for at in range(column.shape[0])]
    vectors = []
    for at, cell in enumerate(cells):
        rows = [slice(NVEC * i + NVEC - 1, NVEC * i + NVEC) for i in range(3)]
        summed = [shared[0, at, row, :] + shared[1, at, row, :] for row in rows]
        vectors.append(jacobi_of(cell, summed))
        for i in range(3):
            jacobi[at, i : i + 1, :] = vectors[at][i]
    apply_pairs(6, column_block, column, cells, vectors, even, odd, fields, moments)


def beside_apply_kernel(
    column, straight, crossed, newest, newest_crossed, even, odd, begun, fields, moments
):
    core = lax.axis_index("gy")
    fields[...] = begun[...]
    cells = [ref[at] for ref in (straight, crossed) for at in range(ref.shape[0])]
    vectors = []
    for at, cell in enumerate(cells):
        y = beside_row(at, core, len(cells))
        summed = newest[y] + newest_crossed[y]
        vectors.append(jacobi_of(cell, [summed[i : i + 1] for i in range(3)]))
    apply_pairs(12, beside_block, column, cells, vectors, even, odd, fields, moments)


def own_vectors(core, cell, i, column, jacobi, shared, shared_last):
    at = 2 * core + cell
    slots = column.shape[-1]
    last = lax.broadcasted_iota(jnp.int32, (NVEC, slots), 0) == NVEC - 1
    rows = slice(NVEC * i, NVEC * i + NVEC)
    vectors = column[at, rows, :]
    current = vectors[NVEC - 1 :]
    jacobi_row = jacobi[at, i : i + 1, :]
    vectors = jnp.where(last, jacobi_row, vectors)
    field = shared[0, at, rows, :] + shared[1, at, rows, :]
    newest = shared_last[0, at, i : i + 1, :] + shared_last[1, at, i : i + 1, :]
    field = jnp.where(last, newest, field)
    scaled = column[at, ROW_POLAR : ROW_POLAR + 1, :] * column[at, ROW_OCC : ROW_OCC + 1, :]
    perm = column[at, ROW_PERM + i : ROW_PERM + i + 1, :]
    return vectors, field, current, jacobi_row, scaled, perm


def gram_kernel(column, jacobi, shared, shared_last, past_res, gram):
    core = lax.axis_index("gy")
    pieces = []
    for cell in range(past_res.shape[2]):
        occ = column[2 * core + cell, ROW_OCC : ROW_OCC + 1, :]
        for i in range(3):
            vectors, field, current, newest, scaled, perm = own_vectors(
                core, cell, i, column, jacobi, shared, shared_last
            )
            old = [past_res[k, i, cell : cell + 1, :] for k in range(NVEC - 1)]
            residual = jnp.concatenate(old + [newest - current], axis=0) * occ
            implied = scaled * (perm + field) - vectors
            pieces.append(jnp.concatenate([residual, implied], axis=0))
    count = 2 * NVEC
    parts = split3(jnp.concatenate(pieces, axis=1))
    many = jnp.concatenate(parts, axis=0)

    def products(left, right):
        return lax.dot_general(
            left, right, (((1,), (1,)), ((), ())), preferred_element_type=F32
        )

    first = products(many, parts[0])
    second = products(many[: 2 * count], parts[1])
    third = products(parts[0], parts[2])
    total = (first[:count] + first[count : 2 * count] + first[2 * count :]) + (
        second[:count] + second[count:] + third
    )
    row = lax.broadcasted_iota(jnp.int32, (count, count * count), 0)
    lane = lax.broadcasted_iota(jnp.int32, (count, count * count), 1)
    spread = (lax.rem(lane, count) == row).astype(F32).astype(BF16)
    wide = jnp.dot(
        jnp.concatenate(split3(total), axis=0), spread, preferred_element_type=F32
    )
    wide = wide[:count] + wide[count : 2 * count] + wide[2 * count :]
    flat = jnp.sum(jnp.where(lane // count == row, wide, 0.0), axis=0, keepdims=True)
    half = count * count // 2
    gram[0:1, :] = flat[:, :half]
    gram[1:2, :] = flat[:, half:]


def solve_ones(matrix):
    size = len(matrix)
    lower = [[None] * size for _ in range(size)]
    inverse = [None] * size
    scaled = [[None] * size for _ in range(size)]
    for j in range(size):
        for i in range(j, size):
            value = matrix[i][j]
            for k in range(j):
                value = value - scaled[i][k] * lower[j][k]
            scaled[i][j] = value
        inverse[j] = 1.0 / scaled[j][j]
        for i in range(j + 1, size):
            lower[i][j] = scaled[i][j] * inverse[j]
    forward = []
    for i in range(size):
        value = jnp.ones_like(inverse[0])
        for k in range(i):
            value = value - lower[i][k] * forward[k]
        forward.append(value)
    backward = [None] * size
    for i in reversed(range(size)):
        value = forward[i] * inverse[i]
        for k in range(i + 1, size):
            value = value - lower[k][i] * backward[k]
        backward[i] = value
    total = sum(backward[1:], backward[0])
    return [value / total for value in backward]


def finish_kernel(partials, column, jacobi, shared, shared_last, dipoles, weights):
    core = lax.axis_index("gy")
    slots = column.shape[-1]
    lanes = partials.shape[-1]
    summed = partials[0]
    for k in range(1, partials.shape[0]):
        summed = summed + partials[k]

    def entry(k, j):
        flat = k * 2 * NVEC + j
        row, lane = flat // lanes, flat % lanes
        return jnp.broadcast_to(summed[row : row + 1, lane : lane + 1], (1, lanes))

    first = [[entry(j, k) if j <= k else None for j in range(NVEC)] for k in range(NVEC)]
    early = solve_ones(first)
    mixed = []
    for k in range(1, NVEC):
        value = early[0] * entry(k, NVEC)
        for m in range(1, NVEC):
            value = value + early[m] * entry(k, NVEC + m)
        mixed.append(value)
    square = None
    for m in range(NVEC):
        value = 0.5 * early[m] * entry(NVEC + m, NVEC + m)
        for n in range(m + 1, NVEC):
            value = value + early[n] * entry(NVEC + m, NVEC + n)
        value = early[m] * value
        square = value if square is None else square + value
    second = [
        [first[k][j] if j <= k else None for j in range(1, NVEC)] + [None]
        for k in range(1, NVEC)
    ]
    second.append(mixed + [2.0 * square])
    late = solve_ones(second)

    sub = lax.broadcasted_iota(jnp.int32, (NVEC, lanes), 0)
    lane = lax.broadcasted_iota(jnp.int32, (1, lanes), 1)
    early_column = jnp.zeros((NVEC, lanes), F32)
    late_column = jnp.zeros((NVEC, lanes), F32)
    row = jnp.zeros((1, lanes), F32)
    for k in range(NVEC):
        early_column = jnp.where(sub == k, early[k], early_column)
        if k:
            late_column = jnp.where(sub == k, late[k - 1], late_column)
        row = jnp.where(lane == k, late[k], row)
    weights[...] = row[:, :NVEC]
    reach = slots // lanes
    early_column = jnp.concatenate([early_column] * reach, axis=1)
    late_column = jnp.concatenate([late_column] * reach, axis=1)
    last = jnp.concatenate([late[NVEC - 1]] * reach, axis=1)
    for cell in range(dipoles.shape[1]):
        for i in range(3):
            vectors, field, current, newest, scaled, perm = own_vectors(
                core, cell, i, column, jacobi, shared, shared_last
            )
            induced = jnp.sum(early_column * field, axis=0, keepdims=True)
            output = scaled * (perm + induced)
            kept = jnp.sum(late_column * vectors, axis=0, keepdims=True)
            dipoles[i, cell : cell + 1, :] = kept + last * output


def call(kernel, out_shape, operands, specs=None, scratch=(), megabytes=16, flags=None):
    single = not isinstance(out_shape, (list, tuple))
    outs = [out_shape] if single else list(out_shape)
    result = pl.pallas_call(
        kernel,
        out_shape=outs,
        in_specs=specs or [vmem() for _ in operands],
        out_specs=[vmem() for _ in outs],
        scratch_shapes=list(scratch),
        compiler_params=pltpu.CompilerParams(vmem_limit_bytes=megabytes << 20, flags=flags),
    )(*operands)
    return result[0] if single else result


def shape_of(*dims, dtype=F32):
    return jax.ShapeDtypeStruct(dims, dtype)


def sideways(block):
    count = lax.axis_size(GX)
    cores = lax.axis_size("gy")
    received = []
    for other in (0, 1):
        route = []
        for x in range(count):
            for core in range(cores):
                source = (x - 1 + 2 * core) % count
                route.append((source * cores + (core + other) % cores, x * cores + core))
        received.append(lax.ppermute(block, GX + ("gy",), route))
    return received


def exchanged(block, axes):
    size = lax.axis_size(axes)
    many = jnp.broadcast_to(block[None], (size,) + block.shape)
    return lax.all_to_all(many, axes, 0, 0)


def body(
    positions, polarizability, tile_counts, molecules, perm_field, dipoles, past_out, past_res
):
    own_cells, slots = positions.shape[1], positions.shape[-1]
    cells = 2 * own_cells
    by_comp = [jnp.swapaxes(x[0], 0, 1) for x in (positions, perm_field, dipoles)]
    past_out, past_res = [jnp.moveaxis(x[0], 0, 2) for x in (past_out, past_res)]
    operands = (
        tile_counts[0], by_comp[0], polarizability[0], molecules[0], by_comp[1], by_comp[2], past_out
    )
    packed, groups = call(
        pack_kernel,
        [shape_of(own_cells, ROWS, slots), shape_of(8, slots)],
        [pltpu.with_memory_space_constraint(x, pltpu.HBM) for x in operands],
        [pl.BlockSpec(memory_space=pltpu.HBM)] * 7,
        scratch=[pltpu.SMEM(operands[0].shape, jnp.int32)]
        + [pltpu.VMEM(x.shape, x.dtype) for x in operands[1:]]
        + [pltpu.SemaphoreType.DMA((7,))],
    )
    straight, crossed = sideways(packed)
    column = lax.all_gather(packed, "gy").reshape(cells, ROWS, slots)
    scratch = [
        pltpu.VMEM((cells, 2 * COMPS * NVEC, slots), BF16),
        pltpu.VMEM((cells, slots, 64), BF16),
        pltpu.VMEM((cells, slots, 64), F32),
    ]

    def pair_shapes(count):
        return [shape_of(count // 2, 4, slots, slots, dtype=BF16)] * 2

    fields_shape = shape_of(cells, 3 * NVEC, slots)
    begun, *own_pairs = call(
        own_pairs_kernel,
        [fields_shape] + pair_shapes(6),
        (column, groups),
        scratch=scratch + [pltpu.VMEM((6, slots, slots), F32)],
    )
    last_shape = shape_of(cells, 3, slots)
    partial, newest, *beside_pairs = call(
        beside_pairs_kernel,
        [fields_shape, last_shape] + pair_shapes(12),
        (column, straight, crossed, begun),
        scratch=scratch + [pltpu.VMEM((12, slots, slots), F32)],
    )
    newest, newest_crossed = sideways(newest)
    shared = lax.all_gather(partial, "gy")
    scratch = [pltpu.VMEM((cells, 2 * COMPS, slots), BF16)]
    jacobi, begun = call(
        own_apply_kernel, [last_shape, last_shape], (column, shared, *own_pairs), scratch=scratch
    )
    partial = call(
        beside_apply_kernel,
        last_shape,
        (column, straight, crossed, newest, newest_crossed, *beside_pairs, begun),
        scratch=scratch,
    )
    shared_last = lax.all_gather(partial, "gy")
    gram = call(
        gram_kernel,
        shape_of(2, 2 * NVEC * NVEC),
        (column, jacobi, shared, shared_last, past_res),
    )
    gram = jnp.sum(exchanged(gram, ("gx_1", "gy")), axis=0)
    partials = exchanged(gram, ("gx_0",))
    following, weights = call(
        finish_kernel,
        [shape_of(3, own_cells, slots), shape_of(1, NVEC)],
        (partials, column, jacobi, shared, shared_last),
    )
    return (jnp.swapaxes(following, 0, 1)[None], weights.reshape(NVEC))


def solution(mesh):
    torus = Mesh(
        mesh.devices.reshape(mesh.shape["box"], TORUS_Z, TORUS_X, mesh.shape["gy"]),
        ("box", "gx_0", "gx_1", "gy"),
    )
    return jax.shard_map(
        body,
        mesh=torus,
        in_specs=(
            P(BOX_GX, "gy", None, None),
            P(BOX_GX, "gy", None),
            P(BOX_GX, "gy", None),
            P(BOX_GX, "gy", None),
            P(BOX_GX, "gy", None, None),
            P(BOX_GX, "gy", None, None),
            P(BOX_GX, "gy", None, None, None),
            P(BOX_GX, "gy", None, None, None),
        ),
        out_specs=(P(BOX_GX, "gy", None, None), P("box")),
        check_vma=False,
    )
```

```python
import functools

import jax
import jax.numpy as jnp
from jax import lax
from jax.experimental import pallas as pl
from jax.experimental.pallas import tpu as pltpu
from jax.sharding import Mesh
from jax.sharding import PartitionSpec as P

GX = ("gx_0", "gx_1")
BOX_GX = ("box", "gx_0", "gx_1")
TORUS_Z = 16
TORUS_X = 8

CELL_SIDE = 9.0
CUTOFF_SQ = 81.0
SOFTENING = 0.25
THOLE_DAMP = 0.39
LN2 = 0.6931471805599453

NVEC = 8
ROW_XYZ = 24
ROW_POLAR = 27
ROW_OCC = 28
ROW_PERM = 29
ROWS = 32
COMPS = 16
CHUNK = 16
F32 = jnp.float32
BF16 = jnp.bfloat16


def vmem():
    return pl.BlockSpec(memory_space=pltpu.VMEM)


def smem():
    return pl.BlockSpec(memory_space=pltpu.SMEM)


def split3(value):
    first = value.astype(BF16)
    rest = value - first.astype(F32)
    second = rest.astype(BF16)
    third = (rest - second.astype(F32)).astype(BF16)
    return first, second, third


def split2(value):
    first = value.astype(BF16)
    return first, (value - first.astype(F32)).astype(BF16)


def pack_kernel(*refs):
    sources, packed, groups = refs[:7], refs[7], refs[8]
    held, semaphores = refs[9:16], refs[16]
    copies = [
        pltpu.make_async_copy(source, target, semaphores.at[at])
        for at, (source, target) in enumerate(zip(sources, held))
    ]
    for copy in copies:
        copy.start()
    for copy in copies:
        copy.wait()
    counts, positions, polarity, molecules, permanent, dipoles, past_out = held
    cells, slots = polarity.shape
    tiles = sources[0].shape[1]
    tile = slots // tiles
    slot = lax.broadcasted_iota(jnp.int32, (1, slots), 1)
    groups[...] = jnp.zeros(groups.shape, F32)
    for cell in range(cells):
        occ = (slot < counts[cell, 0]).astype(F32)
        for t in range(1, tiles):
            inside = (slot - t * tile < counts[cell, t]).astype(F32)
            occ = jnp.where(slot >= t * tile, inside, occ)
        at = slice(cell, cell + 1)
        for comp in range(3):
            for k in range(NVEC - 1):
                row = comp * NVEC + k
                packed[cell, row : row + 1, :] = past_out[k, comp, at, :] * occ
            row = comp * NVEC + NVEC - 1
            packed[cell, row : row + 1, :] = dipoles[comp, at, :] * occ
            centre = 0.5 * CELL_SIDE if comp < 2 else CELL_SIDE
            row = (positions[comp, at, :] - centre) * (1.0 / CELL_SIDE)
            packed[cell, ROW_XYZ + comp : ROW_XYZ + comp + 1, :] = row
            packed[cell, ROW_PERM + comp : ROW_PERM + comp + 1, :] = permanent[comp, at, :]
        packed[cell, ROW_POLAR : ROW_POLAR + 1, :] = polarity[at, :]
        packed[cell, ROW_OCC : ROW_OCC + 1, :] = occ
        groups[at, :] = molecules[at, :].astype(F32)


def source_moments(coords, vectors):
    vx, vy, vz = [v * (1.0 / CELL_SIDE**3) for v in vectors]
    dot = coords[0] * vx + coords[1] * vy + coords[2] * vz
    comps = [coords[i] * dot for i in range(3)]
    comps += [coords[i] * v for i in range(3) for v in (vx, vy, vz)]
    return comps + [dot, vx, vy, vz]


def fields_of(moments, isotropic, target):
    along = target[0] * moments[13] + target[1] * moments[14] + target[2] * moments[15]
    shared = moments[12] - along
    out = []
    for i in range(3):
        part = moments[i] - target[i] * shared
        for j in range(3):
            part = part - target[j] * moments[3 + 3 * i + j]
        out.append(3.0 * part - isotropic[i])
    return out


def beside_block(index, core, cells):
    source, step = index // 3, index % 3 - 1
    return source, (source - step) % cells, 0, (2 * core - 1).astype(F32), step, False


def column_block(index, core, cells):
    own_at, step = index // 3, index % 3 - 1
    target = 2 * core + own_at
    return lax.rem(target + step + cells, cells), target, own_at, 0.0, step, step == 0


def place_of(column, block):
    _, target, _, move_x, step, _ = block
    x = column[target, ROW_XYZ : ROW_XYZ + 1, :] - move_x
    y = column[target, ROW_XYZ + 1 : ROW_XYZ + 2, :] - float(step)
    return x, y, column[target, ROW_XYZ + 2 : ROW_XYZ + 3, :]


def filled_rows(rows, count):
    slots = rows[0].shape[-1]
    return jnp.concatenate(rows + [jnp.zeros((count - len(rows), slots), F32)], axis=0)


def paired_parts(value, order):
    parts = [part.astype(F32) for part in split3(value)]
    blank = jnp.zeros_like(value)
    return [parts[at] for at in order] + [blank]


def pair_loop(count, block_at, column, groups, fields, even, odd, moments, feats, columns, square):
    cells, slots = column.shape[0], column.shape[-1]
    core = lax.axis_index("gy")

    def info(index):
        return block_at(index, core, cells)

    def distances(index):
        block = info(index)
        x, y, z = place_of(column, block)
        norm = x * x + y * y + z * z
        rows = filled_rows([-2.0 * x, -2.0 * y, -2.0 * z, norm, jnp.ones_like(norm)], 8)
        rhs = jnp.concatenate(
            [jnp.zeros_like(rows)] + paired_parts(rows, (0, 0, 0, 1, 1, 2)), axis=0
        ).astype(BF16)
        square[index] = jnp.dot(feats[block[0]], rhs, preferred_element_type=F32)

    def produce(index, out, at):
        block = info(index)
        source, target, own_at = block[:3]
        scale = lax.rsqrt(column[target, ROW_POLAR : ROW_POLAR + 1, :])
        scale = scale * (-THOLE_DAMP * CELL_SIDE**3 / LN2)
        if block[5]:
            group = groups[own_at : own_at + 1, :]
        for chunk in range(slots // CHUNK):
            part = slice(chunk * CHUNK, (chunk + 1) * CHUNK)
            near = columns[source, part, :]
            squared = square[index, part, :]
            inverse = lax.rsqrt(squared)
            inverse_sq = inverse * inverse
            exponent = (squared * squared * inverse) * (near[:, 0:1] * scale)
            damping = jnp.exp2(exponent)
            taper = jnp.maximum(1.0 - squared, 0.0)
            weight = (taper * taper) * (inverse_sq * inverse)
            if block[5]:
                weight = jnp.where(near[:, 1:2] == group, 0.0, weight)
            undamped = 1.0 - damping
            isotropic = weight * undamped
            tensorial = (weight * inverse_sq) * (undamped + (LN2 * exponent) * damping)
            for k, value in ((0, tensorial), (2, isotropic)):
                out[at, k, part, :] = value.astype(BF16)
                rest = value - out[at, k, part, :].astype(F32)
                out[at, k + 1, part, :] = rest.astype(BF16)

    def apply(index, pairs, at):
        block = info(index)
        lhs = moments[block[0]]
        size = COMPS * NVEC
        low, band = size - 4 * NVEC, 4 * NVEC
        first = jnp.dot(lhs, pairs[at, 0], preferred_element_type=F32)
        second = jnp.dot(lhs[:size], pairs[at, 1], preferred_element_type=F32)
        total = first[:size] + first[size:] + second
        iso_lhs = jnp.concatenate([lhs[low:size], lhs[size + low :]], 0)
        first = jnp.dot(iso_lhs, pairs[at, 2], preferred_element_type=F32)
        second = jnp.dot(lhs[low:size], pairs[at, 3], preferred_element_type=F32)
        iso = first[:band] + first[band:] + second
        result = fields_of(
            [total[NVEC * i : NVEC * i + NVEC] for i in range(COMPS)],
            [iso[NVEC * i : NVEC * i + NVEC] for i in range(1, 4)],
            place_of(column, block),
        )
        for i in range(3):
            fields[block[1], NVEC * i : NVEC * i + NVEC, :] += result[i]

    ahead = 2
    for index in range(count + 1):
        for later in range(ahead + 1) if index == 0 else (index + ahead,):
            if later < count:
                distances(later)
        if index < count:
            produce(index, (even, odd)[index % 2], index // 2)
        if index:
            last = index - 1
            apply(last, (even, odd)[last % 2], last // 2)


def load_sources(cells, groups, moments, feats, columns):
    core = lax.axis_index("gy")
    for at, cell in enumerate(cells):
        coords = [cell[ROW_XYZ + i : ROW_XYZ + i + 1] for i in range(3)]
        vectors = [cell[NVEC * i : NVEC * i + NVEC] for i in range(3)]
        stacked = jnp.concatenate(source_moments(coords, vectors), axis=0)
        for part, value in enumerate(split2(stacked)):
            moments[at, part * COMPS * NVEC : (part + 1) * COMPS * NVEC, :] = value
        norm = coords[0] * coords[0] + coords[1] * coords[1] + coords[2] * coords[2]
        norm = norm + SOFTENING / CELL_SIDE**2
        head = [lax.rsqrt(cell[ROW_POLAR : ROW_POLAR + 1])]
        if groups is not None:
            own = jnp.clip(at - 2 * core, 0, 1)
            head.append(groups[pl.ds(own, 1), :])
        rows = filled_rows(coords + [jnp.ones_like(norm), norm], 8)
        tall = jnp.concatenate(
            [filled_rows(head, 8)] + paired_parts(rows, (0, 1, 2, 0, 1, 0)), axis=0
        ).T
        columns[at] = tall
        feats[at] = tall.astype(BF16)


def own_pairs_kernel(column, groups, fields, even, odd, moments, feats, columns, square):
    fields[...] = jnp.zeros(fields.shape, F32)
    load_sources([column[at] for at in range(column.shape[0])], groups, moments, feats, columns)
    pair_loop(6, column_block, column, groups, fields, even, odd, moments, feats, columns, square)


def beside_pairs_kernel(
    column, beside, begun, fields, newest, even, odd, moments, feats, columns, square
):
    fields[...] = begun[...]
    cells = [beside[at] for at in range(beside.shape[0])]
    load_sources(cells, None, moments, feats, columns)
    pair_loop(12, beside_block, column, None, fields, even, odd, moments, feats, columns, square)
    for cell in range(newest.shape[0]):
        for i in range(3):
            row = NVEC * i + NVEC - 1
            newest[cell, i : i + 1, :] = fields[cell, row : row + 1, :]


def jacobi_of(cell, fields):
    scaled = cell[ROW_POLAR : ROW_POLAR + 1] * cell[ROW_OCC : ROW_OCC + 1]
    return [scaled * (cell[ROW_PERM + i : ROW_PERM + i + 1] + fields[i]) for i in range(3)]


def apply_pairs(count, block_at, column, cells, vectors, even, odd, fields, moments):
    core = lax.axis_index("gy")
    for at, (cell, values) in enumerate(zip(cells, vectors)):
        coords = [cell[ROW_XYZ + i : ROW_XYZ + i + 1] for i in range(3)]
        stacked = jnp.concatenate(source_moments(coords, values), axis=0)
        for part, value in enumerate(split2(stacked)):
            moments[at, part * COMPS : (part + 1) * COMPS, :] = value
    for index in range(count):
        block = block_at(index, core, len(cells))
        pairs, at = (even, odd)[index % 2], index // 2
        lhs = moments[block[0]]
        first = jnp.dot(lhs, pairs[at, 0], preferred_element_type=F32)
        second = jnp.dot(lhs[:COMPS], pairs[at, 1], preferred_element_type=F32)
        total = first[:COMPS] + first[COMPS:] + second
        first = jnp.dot(lhs, pairs[at, 2], preferred_element_type=F32)
        second = jnp.dot(lhs[:COMPS], pairs[at, 3], preferred_element_type=F32)
        iso = first[:COMPS] + first[COMPS:] + second
        result = fields_of(
            [total[i : i + 1] for i in range(COMPS)],
            [iso[i : i + 1] for i in range(COMPS - 3, COMPS)],
            place_of(column, block),
        )
        for i in range(3):
            fields[block[1], i : i + 1, :] += result[i]


def own_apply_kernel(column, shared, even, odd, jacobi, fields, moments):
    fields[...] = jnp.zeros(fields.shape, F32)
    cells = [column[at] for at in range(column.shape[0])]
    vectors = []
    for at, cell in enumerate(cells):
        rows = [slice(NVEC * i + NVEC - 1, NVEC * i + NVEC) for i in range(3)]
        summed = [shared[0, at, row, :] + shared[1, at, row, :] for row in rows]
        vectors.append(jacobi_of(cell, summed))
        for i in range(3):
            jacobi[at, i : i + 1, :] = vectors[at][i]
    apply_pairs(6, column_block, column, cells, vectors, even, odd, fields, moments)


def beside_apply_kernel(
    column, beside, newest, newest_crossed, even, odd, begun, fields, moments
):
    fields[...] = begun[...]
    cells = [beside[at] for at in range(beside.shape[0])]
    vectors = []
    for at, cell in enumerate(cells):
        summed = newest[at] + newest_crossed[at]
        vectors.append(jacobi_of(cell, [summed[i : i + 1] for i in range(3)]))
    apply_pairs(12, beside_block, column, cells, vectors, even, odd, fields, moments)


def own_vectors(core, cell, i, column, jacobi, shared, shared_last):
    at = 2 * core + cell
    slots = column.shape[-1]
    last = lax.broadcasted_iota(jnp.int32, (NVEC, slots), 0) == NVEC - 1
    rows = slice(NVEC * i, NVEC * i + NVEC)
    vectors = column[at, rows, :]
    current = vectors[NVEC - 1 :]
    jacobi_row = jacobi[at, i : i + 1, :]
    vectors = jnp.where(last, jacobi_row, vectors)
    field = shared[0, at, rows, :] + shared[1, at, rows, :]
    newest = shared_last[0, at, i : i + 1, :] + shared_last[1, at, i : i + 1, :]
    field = jnp.where(last, newest, field)
    scaled = column[at, ROW_POLAR : ROW_POLAR + 1, :] * column[at, ROW_OCC : ROW_OCC + 1, :]
    perm = column[at, ROW_PERM + i : ROW_PERM + i + 1, :]
    return vectors, field, current, jacobi_row, scaled, perm


def gram_kernel(column, jacobi, shared, shared_last, past_res, gram):
    core = lax.axis_index("gy")
    pieces = []
    for cell in range(past_res.shape[2]):
        occ = column[2 * core + cell, ROW_OCC : ROW_OCC + 1, :]
        for i in range(3):
            vectors, field, current, newest, scaled, perm = own_vectors(
                core, cell, i, column, jacobi, shared, shared_last
            )
            old = [past_res[k, i, cell : cell + 1, :] for k in range(NVEC - 1)]
            residual = jnp.concatenate(old + [newest - current], axis=0) * occ
            implied = scaled * (perm + field) - vectors
            pieces.append(jnp.concatenate([residual, implied], axis=0))
    count = 2 * NVEC
    parts = split3(jnp.concatenate(pieces, axis=1))
    many = jnp.concatenate(parts, axis=0)

    def products(left, right):
        return lax.dot_general(
            left, right, (((1,), (1,)), ((), ())), preferred_element_type=F32
        )

    first = products(many, parts[0])
    second = products(many[: 2 * count], parts[1])
    third = products(parts[0], parts[2])
    total = (first[:count] + first[count : 2 * count] + first[2 * count :]) + (
        second[:count] + second[count:] + third
    )
    row = lax.broadcasted_iota(jnp.int32, (count, count * count), 0)
    lane = lax.broadcasted_iota(jnp.int32, (count, count * count), 1)
    spread = (lax.rem(lane, count) == row).astype(F32).astype(BF16)
    wide = jnp.dot(
        jnp.concatenate(split3(total), axis=0), spread, preferred_element_type=F32
    )
    wide = wide[:count] + wide[count : 2 * count] + wide[2 * count :]
    flat = jnp.sum(jnp.where(lane // count == row, wide, 0.0), axis=0, keepdims=True)
    half = count * count // 2
    gram[0:1, :] = flat[:, :half]
    gram[1:2, :] = flat[:, half:]


def solve_ones(matrix):
    size = len(matrix)
    lower = [[None] * size for _ in range(size)]
    inverse = [None] * size
    scaled = [[None] * size for _ in range(size)]
    for j in range(size):
        for i in range(j, size):
            value = matrix[i][j]
            for k in range(j):
                value = value - scaled[i][k] * lower[j][k]
            scaled[i][j] = value
        inverse[j] = 1.0 / scaled[j][j]
        for i in range(j + 1, size):
            lower[i][j] = scaled[i][j] * inverse[j]
    forward = []
    for i in range(size):
        value = jnp.ones_like(inverse[0])
        for k in range(i):
            value = value - lower[i][k] * forward[k]
        forward.append(value)
    backward = [None] * size
    for i in reversed(range(size)):
        value = forward[i] * inverse[i]
        for k in range(i + 1, size):
            value = value - lower[k][i] * backward[k]
        backward[i] = value
    total = sum(backward[1:], backward[0])
    return [value / total for value in backward]


def finish_kernel(partials, column, jacobi, shared, shared_last, dipoles, weights):
    core = lax.axis_index("gy")
    slots = column.shape[-1]
    lanes = partials.shape[-1]
    summed = partials[0]
    for k in range(1, partials.shape[0]):
        summed = summed + partials[k]

    def entry(k, j):
        flat = k * 2 * NVEC + j
        row, lane = flat // lanes, flat % lanes
        return jnp.broadcast_to(summed[row : row + 1, lane : lane + 1], (1, lanes))

    first = [[entry(j, k) if j <= k else None for j in range(NVEC)] for k in range(NVEC)]
    early = solve_ones(first)
    mixed = []
    for k in range(1, NVEC):
        value = early[0] * entry(k, NVEC)
        for m in range(1, NVEC):
            value = value + early[m] * entry(k, NVEC + m)
        mixed.append(value)
    square = None
    for m in range(NVEC):
        value = 0.5 * early[m] * entry(NVEC + m, NVEC + m)
        for n in range(m + 1, NVEC):
            value = value + early[n] * entry(NVEC + m, NVEC + n)
        value = early[m] * value
        square = value if square is None else square + value
    second = [
        [first[k][j] if j <= k else None for j in range(1, NVEC)] + [None]
        for k in range(1, NVEC)
    ]
    second.append(mixed + [2.0 * square])
    late = solve_ones(second)

    sub = lax.broadcasted_iota(jnp.int32, (NVEC, lanes), 0)
    lane = lax.broadcasted_iota(jnp.int32, (1, lanes), 1)
    early_column = jnp.zeros((NVEC, lanes), F32)
    late_column = jnp.zeros((NVEC, lanes), F32)
    row = jnp.zeros((1, lanes), F32)
    for k in range(NVEC):
        early_column = jnp.where(sub == k, early[k], early_column)
        if k:
            late_column = jnp.where(sub == k, late[k - 1], late_column)
        row = jnp.where(lane == k, late[k], row)
    weights[...] = row[:, :NVEC]
    reach = slots // lanes
    early_column = jnp.concatenate([early_column] * reach, axis=1)
    late_column = jnp.concatenate([late_column] * reach, axis=1)
    last = jnp.concatenate([late[NVEC - 1]] * reach, axis=1)
    for cell in range(dipoles.shape[1]):
        for i in range(3):
            vectors, field, current, newest, scaled, perm = own_vectors(
                core, cell, i, column, jacobi, shared, shared_last
            )
            induced = jnp.sum(early_column * field, axis=0, keepdims=True)
            output = scaled * (perm + induced)
            kept = jnp.sum(late_column * vectors, axis=0, keepdims=True)
            dipoles[i, cell : cell + 1, :] = kept + last * output


def call(kernel, out_shape, operands, specs=None, scratch=(), megabytes=16, flags=None):
    single = not isinstance(out_shape, (list, tuple))
    outs = [out_shape] if single else list(out_shape)
    result = pl.pallas_call(
        kernel,
        out_shape=outs,
        in_specs=specs or [vmem() for _ in operands],
        out_specs=[vmem() for _ in outs],
        scratch_shapes=list(scratch),
        compiler_params=pltpu.CompilerParams(vmem_limit_bytes=megabytes << 20, flags=flags),
    )(*operands)
    return result[0] if single else result


def shape_of(*dims, dtype=F32):
    return jax.ShapeDtypeStruct(dims, dtype)


def sideways(block, others):
    count = lax.axis_size(GX)
    cores = lax.axis_size("gy")
    received = []
    for other in others:
        route = []
        for x in range(count):
            for core in range(cores):
                source = (x - 1 + 2 * core) % count
                route.append((source * cores + (core + other) % cores, x * cores + core))
        received.append(lax.ppermute(block, GX + ("gy",), route))
    return received


def exchanged(block, axes):
    size = lax.axis_size(axes)
    many = jnp.broadcast_to(block[None], (size,) + block.shape)
    return lax.all_to_all(many, axes, 0, 0)


def body(
    positions, polarizability, tile_counts, molecules, perm_field, dipoles, past_out, past_res
):
    own_cells, slots = positions.shape[1], positions.shape[-1]
    cells = 2 * own_cells
    by_comp = [jnp.swapaxes(x[0], 0, 1) for x in (positions, perm_field, dipoles)]
    past_out, past_res = [jnp.moveaxis(x[0], 0, 2) for x in (past_out, past_res)]
    operands = (
        tile_counts[0], by_comp[0], polarizability[0], molecules[0], by_comp[1], by_comp[2], past_out
    )
    packed, groups = call(
        pack_kernel,
        [shape_of(own_cells, ROWS, slots), shape_of(8, slots)],
        [pltpu.with_memory_space_constraint(x, pltpu.HBM) for x in operands],
        [pl.BlockSpec(memory_space=pltpu.HBM)] * 7,
        scratch=[pltpu.SMEM(operands[0].shape, jnp.int32)]
        + [pltpu.VMEM(x.shape, x.dtype) for x in operands[1:]]
        + [pltpu.SemaphoreType.DMA((7,))],
    )
    column = lax.all_gather(packed, "gy").reshape(cells, ROWS, slots)
    (beside,) = sideways(column, (0,))
    scratch = [
        pltpu.VMEM((cells, 2 * COMPS * NVEC, slots), BF16),
        pltpu.VMEM((cells, slots, 64), BF16),
        pltpu.VMEM((cells, slots, 64), F32),
    ]

    def pair_shapes(count):
        return [shape_of(count // 2, 4, slots, slots, dtype=BF16)] * 2

    fields_shape = shape_of(cells, 3 * NVEC, slots)
    begun, *own_pairs = call(
        own_pairs_kernel,
        [fields_shape] + pair_shapes(6),
        (column, groups),
        scratch=scratch + [pltpu.VMEM((6, slots, slots), F32)],
    )
    last_shape = shape_of(cells, 3, slots)
    partial, newest, *beside_pairs = call(
        beside_pairs_kernel,
        [fields_shape, last_shape] + pair_shapes(12),
        (column, beside, begun),
        scratch=scratch + [pltpu.VMEM((12, slots, slots), F32)],
    )
    newest, newest_crossed = sideways(newest, (0, 1))
    shared = lax.all_gather(partial, "gy")
    scratch = [pltpu.VMEM((cells, 2 * COMPS, slots), BF16)]
    jacobi, begun = call(
        own_apply_kernel, [last_shape, last_shape], (column, shared, *own_pairs), scratch=scratch
    )
    partial = call(
        beside_apply_kernel,
        last_shape,
        (column, beside, newest, newest_crossed, *beside_pairs, begun),
        scratch=scratch,
    )
    shared_last = lax.all_gather(partial, "gy")
    gram = call(
        gram_kernel,
        shape_of(2, 2 * NVEC * NVEC),
        (column, jacobi, shared, shared_last, past_res),
    )
    gram = jnp.sum(exchanged(gram, ("gx_1", "gy")), axis=0)
    partials = exchanged(gram, ("gx_0",))
    following, weights = call(
        finish_kernel,
        [shape_of(3, own_cells, slots), shape_of(1, NVEC)],
        (partials, column, jacobi, shared, shared_last),
    )
    return (jnp.swapaxes(following, 0, 1)[None], weights.reshape(NVEC))


def solution(mesh):
    torus = Mesh(
        mesh.devices.reshape(mesh.shape["box"], TORUS_Z, TORUS_X, mesh.shape["gy"]),
        ("box", "gx_0", "gx_1", "gy"),
    )
    return jax.shard_map(
        body,
        mesh=torus,
        in_specs=(
            P(BOX_GX, "gy", None, None),
            P(BOX_GX, "gy", None),
            P(BOX_GX, "gy", None),
            P(BOX_GX, "gy", None),
            P(BOX_GX, "gy", None, None),
            P(BOX_GX, "gy", None, None),
            P(BOX_GX, "gy", None, None, None),
            P(BOX_GX, "gy", None, None, None),
        ),
        out_specs=(P(BOX_GX, "gy", None, None), P("box")),
        check_vma=False,
    )
```

```python
import functools

import jax
import jax.numpy as jnp
from jax import lax
from jax.experimental import pallas as pl
from jax.experimental.pallas import tpu as pltpu
from jax.sharding import Mesh
from jax.sharding import PartitionSpec as P

GX = ("gx_0", "gx_1")
BOX_GX = ("box", "gx_0", "gx_1")
TORUS_Z = 16
TORUS_X = 8

CELL_SIDE = 9.0
CUTOFF_SQ = 81.0
SOFTENING = 0.25
THOLE_DAMP = 0.39
LN2 = 0.6931471805599453

NVEC = 8
ROW_XYZ = 24
ROW_POLAR = 27
ROW_OCC = 28
ROW_PERM = 29
ROWS = 32
COMPS = 16
CHUNK = 16
F32 = jnp.float32
BF16 = jnp.bfloat16


def vmem():
    return pl.BlockSpec(memory_space=pltpu.VMEM)


def smem():
    return pl.BlockSpec(memory_space=pltpu.SMEM)


def split3(value):
    first = value.astype(BF16)
    rest = value - first.astype(F32)
    second = rest.astype(BF16)
    third = (rest - second.astype(F32)).astype(BF16)
    return first, second, third


def split2(value):
    first = value.astype(BF16)
    return first, (value - first.astype(F32)).astype(BF16)


def pack_kernel(*refs):
    sources, packed, groups = refs[:7], refs[7], refs[8]
    held, semaphores = refs[9:16], refs[16]
    copies = [
        pltpu.make_async_copy(source, target, semaphores.at[at])
        for at, (source, target) in enumerate(zip(sources, held))
    ]
    for copy in copies:
        copy.start()
    for copy in copies:
        copy.wait()
    counts, positions, polarity, molecules, permanent, dipoles, past_out = held
    cells, slots = polarity.shape
    tiles = sources[0].shape[1]
    tile = slots // tiles
    slot = lax.broadcasted_iota(jnp.int32, (1, slots), 1)
    groups[...] = jnp.zeros(groups.shape, F32)
    for cell in range(cells):
        occ = (slot < counts[cell, 0]).astype(F32)
        for t in range(1, tiles):
            inside = (slot - t * tile < counts[cell, t]).astype(F32)
            occ = jnp.where(slot >= t * tile, inside, occ)
        at = slice(cell, cell + 1)
        for comp in range(3):
            for k in range(NVEC - 1):
                row = comp * NVEC + k
                packed[cell, row : row + 1, :] = past_out[k, comp, at, :] * occ
            row = comp * NVEC + NVEC - 1
            packed[cell, row : row + 1, :] = dipoles[comp, at, :] * occ
            centre = 0.5 * CELL_SIDE if comp < 2 else CELL_SIDE
            row = (positions[comp, at, :] - centre) * (1.0 / CELL_SIDE)
            packed[cell, ROW_XYZ + comp : ROW_XYZ + comp + 1, :] = row
            packed[cell, ROW_PERM + comp : ROW_PERM + comp + 1, :] = permanent[comp, at, :]
        packed[cell, ROW_POLAR : ROW_POLAR + 1, :] = polarity[at, :]
        packed[cell, ROW_OCC : ROW_OCC + 1, :] = occ
        groups[at, :] = molecules[at, :].astype(F32)


def source_moments(coords, vectors):
    vx, vy, vz = [v * (1.0 / CELL_SIDE**3) for v in vectors]
    dot = coords[0] * vx + coords[1] * vy + coords[2] * vz
    comps = [coords[i] * dot for i in range(3)]
    comps += [coords[i] * v for i in range(3) for v in (vx, vy, vz)]
    return comps + [dot, vx, vy, vz]


def fields_of(moments, isotropic, target):
    along = target[0] * moments[13] + target[1] * moments[14] + target[2] * moments[15]
    shared = moments[12] - along
    out = []
    for i in range(3):
        part = moments[i] - target[i] * shared
        for j in range(3):
            part = part - target[j] * moments[3 + 3 * i + j]
        out.append(3.0 * part - isotropic[i])
    return out


def beside_block(index, core, cells):
    source, step = index // 3, index % 3 - 1
    return source, (source - step) % cells, 0, (2 * core - 1).astype(F32), step, False


def column_block(index, core, cells):
    own_at, step = index // 3, index % 3 - 1
    target = 2 * core + own_at
    return lax.rem(target + step + cells, cells), target, own_at, 0.0, step, step == 0


def place_of(column, block):
    _, target, _, move_x, step, _ = block
    x = column[target, ROW_XYZ : ROW_XYZ + 1, :] - move_x
    y = column[target, ROW_XYZ + 1 : ROW_XYZ + 2, :] - float(step)
    return x, y, column[target, ROW_XYZ + 2 : ROW_XYZ + 3, :]


def filled_rows(rows, count):
    slots = rows[0].shape[-1]
    return jnp.concatenate(rows + [jnp.zeros((count - len(rows), slots), F32)], axis=0)


def paired_parts(value, order):
    parts = [part.astype(F32) for part in split3(value)]
    blank = jnp.zeros_like(value)
    return [parts[at] for at in order] + [blank]


def pair_loop(count, block_at, column, groups, fields, even, odd, moments, feats, columns, square):
    cells, slots = column.shape[0], column.shape[-1]
    core = lax.axis_index("gy")

    def info(index):
        return block_at(index, core, cells)

    def distances(index):
        block = info(index)
        x, y, z = place_of(column, block)
        norm = x * x + y * y + z * z
        rows = filled_rows([-2.0 * x, -2.0 * y, -2.0 * z, norm, jnp.ones_like(norm)], 8)
        rhs = jnp.concatenate(
            [jnp.zeros_like(rows)] + paired_parts(rows, (0, 0, 0, 1, 1, 2)), axis=0
        ).astype(BF16)
        square[index] = jnp.dot(feats[block[0]], rhs, preferred_element_type=F32)

    def produce(index, out, at):
        block = info(index)
        source, target, own_at = block[:3]
        scale = lax.rsqrt(column[target, ROW_POLAR : ROW_POLAR + 1, :])
        scale = scale * (-THOLE_DAMP * CELL_SIDE**3 / LN2)
        if block[5]:
            group = groups[own_at : own_at + 1, :]
        for chunk in range(slots // CHUNK):
            part = slice(chunk * CHUNK, (chunk + 1) * CHUNK)
            near = columns[source, part, :]
            squared = square[index, part, :]
            inverse = lax.rsqrt(squared)
            inverse_sq = inverse * inverse
            exponent = (squared * squared * inverse) * (near[:, 0:1] * scale)
            damping = jnp.exp2(exponent)
            taper = jnp.maximum(1.0 - squared, 0.0)
            weight = (taper * taper) * (inverse_sq * inverse)
            if block[5]:
                weight = jnp.where(near[:, 1:2] == group, 0.0, weight)
            undamped = 1.0 - damping
            isotropic = weight * undamped
            tensorial = (weight * inverse_sq) * (undamped + (LN2 * exponent) * damping)
            for k, value in ((0, tensorial), (2, isotropic)):
                out[at, k, part, :] = value.astype(BF16)
                rest = value - out[at, k, part, :].astype(F32)
                out[at, k + 1, part, :] = rest.astype(BF16)

    def apply(index, pairs, at):
        block = info(index)
        lhs = moments[block[0]]
        size = COMPS * NVEC
        low, band = size - 4 * NVEC, 4 * NVEC
        first = jnp.dot(lhs, pairs[at, 0], preferred_element_type=F32)
        second = jnp.dot(lhs[:size], pairs[at, 1], preferred_element_type=F32)
        total = first[:size] + first[size:] + second
        iso_lhs = jnp.concatenate([lhs[low:size], lhs[size + low :]], 0)
        first = jnp.dot(iso_lhs, pairs[at, 2], preferred_element_type=F32)
        second = jnp.dot(lhs[low:size], pairs[at, 3], preferred_element_type=F32)
        iso = first[:band] + first[band:] + second
        result = fields_of(
            [total[NVEC * i : NVEC * i + NVEC] for i in range(COMPS)],
            [iso[NVEC * i : NVEC * i + NVEC] for i in range(1, 4)],
            place_of(column, block),
        )
        for i in range(3):
            fields[block[1], NVEC * i : NVEC * i + NVEC, :] += result[i]

    ahead = 2
    for index in range(count + 1):
        for later in range(ahead + 1) if index == 0 else (index + ahead,):
            if later < count:
                distances(later)
        if index < count:
            produce(index, (even, odd)[index % 2], index // 2)
        if index:
            last = index - 1
            apply(last, (even, odd)[last % 2], last // 2)


def load_sources(cells, groups, moments, feats, columns):
    core = lax.axis_index("gy")
    for at, cell in enumerate(cells):
        coords = [cell[ROW_XYZ + i : ROW_XYZ + i + 1] for i in range(3)]
        vectors = [cell[NVEC * i : NVEC * i + NVEC] for i in range(3)]
        stacked = jnp.concatenate(source_moments(coords, vectors), axis=0)
        for part, value in enumerate(split2(stacked)):
            moments[at, part * COMPS * NVEC : (part + 1) * COMPS * NVEC, :] = value
        norm = coords[0] * coords[0] + coords[1] * coords[1] + coords[2] * coords[2]
        norm = norm + SOFTENING / CELL_SIDE**2
        head = [lax.rsqrt(cell[ROW_POLAR : ROW_POLAR + 1])]
        if groups is not None:
            own = jnp.clip(at - 2 * core, 0, 1)
            head.append(groups[pl.ds(own, 1), :])
        rows = filled_rows(coords + [jnp.ones_like(norm), norm], 8)
        tall = jnp.concatenate(
            [filled_rows(head, 8)] + paired_parts(rows, (0, 1, 2, 0, 1, 0)), axis=0
        ).T
        columns[at] = tall
        feats[at] = tall.astype(BF16)


def own_pairs_kernel(column, groups, fields, even, odd, moments, feats, columns, square):
    fields[...] = jnp.zeros(fields.shape, F32)
    load_sources([column[at] for at in range(column.shape[0])], groups, moments, feats, columns)
    pair_loop(6, column_block, column, groups, fields, even, odd, moments, feats, columns, square)


def beside_pairs_kernel(
    column, beside, begun, fields, newest, even, odd, moments, feats, columns, square
):
    fields[...] = begun[...]
    cells = [beside[at] for at in range(beside.shape[0])]
    load_sources(cells, None, moments, feats, columns)
    pair_loop(12, beside_block, column, None, fields, even, odd, moments, feats, columns, square)
    for cell in range(newest.shape[0]):
        for i in range(3):
            row = NVEC * i + NVEC - 1
            newest[cell, i : i + 1, :] = fields[cell, row : row + 1, :]


def jacobi_of(cell, fields):
    scaled = cell[ROW_POLAR : ROW_POLAR + 1] * cell[ROW_OCC : ROW_OCC + 1]
    return [scaled * (cell[ROW_PERM + i : ROW_PERM + i + 1] + fields[i]) for i in range(3)]


def apply_pairs(count, block_at, column, cells, vectors, even, odd, fields, moments):
    core = lax.axis_index("gy")
    for at, (cell, values) in enumerate(zip(cells, vectors)):
        coords = [cell[ROW_XYZ + i : ROW_XYZ + i + 1] for i in range(3)]
        stacked = jnp.concatenate(source_moments(coords, values), axis=0)
        for part, value in enumerate(split2(stacked)):
            moments[at, part * COMPS : (part + 1) * COMPS, :] = value
    for index in range(count):
        block = block_at(index, core, len(cells))
        pairs, at = (even, odd)[index % 2], index // 2
        lhs = moments[block[0]]
        first = jnp.dot(lhs, pairs[at, 0], preferred_element_type=F32)
        second = jnp.dot(lhs[:COMPS], pairs[at, 1], preferred_element_type=F32)
        total = first[:COMPS] + first[COMPS:] + second
        first = jnp.dot(lhs, pairs[at, 2], preferred_element_type=F32)
        second = jnp.dot(lhs[:COMPS], pairs[at, 3], preferred_element_type=F32)
        iso = first[:COMPS] + first[COMPS:] + second
        result = fields_of(
            [total[i : i + 1] for i in range(COMPS)],
            [iso[i : i + 1] for i in range(COMPS - 3, COMPS)],
            place_of(column, block),
        )
        for i in range(3):
            fields[block[1], i : i + 1, :] += result[i]


def own_apply_kernel(column, shared, even, odd, jacobi, fields, moments):
    fields[...] = jnp.zeros(fields.shape, F32)
    cells = [column[at] for at in range(column.shape[0])]
    vectors = []
    for at, cell in enumerate(cells):
        rows = [slice(NVEC * i + NVEC - 1, NVEC * i + NVEC) for i in range(3)]
        summed = [shared[0, at, row, :] + shared[1, at, row, :] for row in rows]
        vectors.append(jacobi_of(cell, summed))
        for i in range(3):
            jacobi[at, i : i + 1, :] = vectors[at][i]
    apply_pairs(6, column_block, column, cells, vectors, even, odd, fields, moments)


def beside_apply_kernel(
    column, beside, newest, newest_crossed, even, odd, begun, fields, moments
):
    fields[...] = begun[...]
    cells = [beside[at] for at in range(beside.shape[0])]
    vectors = []
    for at, cell in enumerate(cells):
        summed = newest[at] + newest_crossed[at]
        vectors.append(jacobi_of(cell, [summed[i : i + 1] for i in range(3)]))
    apply_pairs(12, beside_block, column, cells, vectors, even, odd, fields, moments)


def own_vectors(core, cell, i, column, jacobi, shared, shared_last):
    at = 2 * core + cell
    slots = column.shape[-1]
    last = lax.broadcasted_iota(jnp.int32, (NVEC, slots), 0) == NVEC - 1
    rows = slice(NVEC * i, NVEC * i + NVEC)
    vectors = column[at, rows, :]
    current = vectors[NVEC - 1 :]
    jacobi_row = jacobi[at, i : i + 1, :]
    vectors = jnp.where(last, jacobi_row, vectors)
    field = shared[0, at, rows, :] + shared[1, at, rows, :]
    newest = shared_last[0, at, i : i + 1, :] + shared_last[1, at, i : i + 1, :]
    field = jnp.where(last, newest, field)
    scaled = column[at, ROW_POLAR : ROW_POLAR + 1, :] * column[at, ROW_OCC : ROW_OCC + 1, :]
    perm = column[at, ROW_PERM + i : ROW_PERM + i + 1, :]
    return vectors, field, current, jacobi_row, scaled, perm


def gram_kernel(column, jacobi, shared, shared_last, past_res, gram):
    core = lax.axis_index("gy")
    pieces = []
    for cell in range(past_res.shape[2]):
        occ = column[2 * core + cell, ROW_OCC : ROW_OCC + 1, :]
        for i in range(3):
            vectors, field, current, newest, scaled, perm = own_vectors(
                core, cell, i, column, jacobi, shared, shared_last
            )
            old = [past_res[k, i, cell : cell + 1, :] for k in range(NVEC - 1)]
            residual = jnp.concatenate(old + [newest - current], axis=0) * occ
            implied = scaled * (perm + field) - vectors
            pieces.append(jnp.concatenate([residual, implied], axis=0))
    count = 2 * NVEC
    parts = split3(jnp.concatenate(pieces, axis=1))
    many = jnp.concatenate(parts, axis=0)

    def products(left, right):
        return lax.dot_general(
            left, right, (((1,), (1,)), ((), ())), preferred_element_type=F32
        )

    first = products(many, parts[0])
    second = products(many[: 2 * count], parts[1])
    third = products(parts[0], parts[2])
    total = (first[:count] + first[count : 2 * count] + first[2 * count :]) + (
        second[:count] + second[count:] + third
    )
    row = lax.broadcasted_iota(jnp.int32, (count, count * count), 0)
    lane = lax.broadcasted_iota(jnp.int32, (count, count * count), 1)
    spread = (lax.rem(lane, count) == row).astype(F32).astype(BF16)
    wide = jnp.dot(
        jnp.concatenate(split3(total), axis=0), spread, preferred_element_type=F32
    )
    wide = wide[:count] + wide[count : 2 * count] + wide[2 * count :]
    flat = jnp.sum(jnp.where(lane // count == row, wide, 0.0), axis=0, keepdims=True)
    half = count * count // 2
    gram[0:1, :] = flat[:, :half]
    gram[1:2, :] = flat[:, half:]


def solve_ones(matrix):
    size = len(matrix)
    lower = [[None] * size for _ in range(size)]
    inverse = [None] * size
    scaled = [[None] * size for _ in range(size)]
    for j in range(size):
        for i in range(j, size):
            value = matrix[i][j]
            for k in range(j):
                value = value - scaled[i][k] * lower[j][k]
            scaled[i][j] = value
        inverse[j] = 1.0 / scaled[j][j]
        for i in range(j + 1, size):
            lower[i][j] = scaled[i][j] * inverse[j]
    forward = []
    for i in range(size):
        value = jnp.ones_like(inverse[0])
        for k in range(i):
            value = value - lower[i][k] * forward[k]
        forward.append(value)
    backward = [None] * size
    for i in reversed(range(size)):
        value = forward[i] * inverse[i]
        for k in range(i + 1, size):
            value = value - lower[k][i] * backward[k]
        backward[i] = value
    total = sum(backward[1:], backward[0])
    return [value / total for value in backward]


def finish_kernel(partials, column, jacobi, shared, shared_last, dipoles, weights):
    core = lax.axis_index("gy")
    slots = column.shape[-1]
    lanes = partials.shape[-1]
    summed = partials[0]
    for k in range(1, partials.shape[0]):
        summed = summed + partials[k]

    def entry(k, j):
        flat = k * 2 * NVEC + j
        row, lane = flat // lanes, flat % lanes
        return jnp.broadcast_to(summed[row : row + 1, lane : lane + 1], (1, lanes))

    first = [[entry(j, k) if j <= k else None for j in range(NVEC)] for k in range(NVEC)]
    early = solve_ones(first)
    mixed = []
    for k in range(1, NVEC):
        value = early[0] * entry(k, NVEC)
        for m in range(1, NVEC):
            value = value + early[m] * entry(k, NVEC + m)
        mixed.append(value)
    square = None
    for m in range(NVEC):
        value = 0.5 * early[m] * entry(NVEC + m, NVEC + m)
        for n in range(m + 1, NVEC):
            value = value + early[n] * entry(NVEC + m, NVEC + n)
        value = early[m] * value
        square = value if square is None else square + value
    second = [
        [first[k][j] if j <= k else None for j in range(1, NVEC)] + [None]
        for k in range(1, NVEC)
    ]
    second.append(mixed + [2.0 * square])
    late = solve_ones(second)

    sub = lax.broadcasted_iota(jnp.int32, (NVEC, lanes), 0)
    lane = lax.broadcasted_iota(jnp.int32, (1, lanes), 1)
    early_column = jnp.zeros((NVEC, lanes), F32)
    late_column = jnp.zeros((NVEC, lanes), F32)
    row = jnp.zeros((1, lanes), F32)
    for k in range(NVEC):
        early_column = jnp.where(sub == k, early[k], early_column)
        if k:
            late_column = jnp.where(sub == k, late[k - 1], late_column)
        row = jnp.where(lane == k, late[k], row)
    weights[...] = row[:, :NVEC]
    reach = slots // lanes
    early_column = jnp.concatenate([early_column] * reach, axis=1)
    late_column = jnp.concatenate([late_column] * reach, axis=1)
    last = jnp.concatenate([late[NVEC - 1]] * reach, axis=1)
    for cell in range(dipoles.shape[1]):
        for i in range(3):
            vectors, field, current, newest, scaled, perm = own_vectors(
                core, cell, i, column, jacobi, shared, shared_last
            )
            induced = jnp.sum(early_column * field, axis=0, keepdims=True)
            output = scaled * (perm + induced)
            kept = jnp.sum(late_column * vectors, axis=0, keepdims=True)
            dipoles[i, cell : cell + 1, :] = kept + last * output


def call(kernel, out_shape, operands, specs=None, scratch=(), megabytes=16, flags=None):
    single = not isinstance(out_shape, (list, tuple))
    outs = [out_shape] if single else list(out_shape)
    result = pl.pallas_call(
        kernel,
        out_shape=outs,
        in_specs=specs or [vmem() for _ in operands],
        out_specs=[vmem() for _ in outs],
        scratch_shapes=list(scratch),
        compiler_params=pltpu.CompilerParams(vmem_limit_bytes=megabytes << 20, flags=flags),
    )(*operands)
    return result[0] if single else result


def shape_of(*dims, dtype=F32):
    return jax.ShapeDtypeStruct(dims, dtype)


def sideways(block, others):
    count = lax.axis_size(GX)
    cores = lax.axis_size("gy")
    received = []
    for other in others:
        route = []
        for x in range(count):
            for core in range(cores):
                source = (x - 1 + 2 * core) % count
                route.append((source * cores + (core + other) % cores, x * cores + core))
        received.append(lax.ppermute(block, GX + ("gy",), route))
    return received


def exchanged(block, axes):
    size = lax.axis_size(axes)
    many = jnp.broadcast_to(block[None], (size,) + block.shape)
    return lax.all_to_all(many, axes, 0, 0)


def body(
    positions, polarizability, tile_counts, molecules, perm_field, dipoles, past_out, past_res
):
    own_cells, slots = positions.shape[1], positions.shape[-1]
    cells = 2 * own_cells
    by_comp = [jnp.swapaxes(x[0], 0, 1) for x in (positions, perm_field, dipoles)]
    past_out, past_res = [jnp.moveaxis(x[0], 0, 2) for x in (past_out, past_res)]
    operands = (
        tile_counts[0], by_comp[0], polarizability[0], molecules[0], by_comp[1], by_comp[2], past_out
    )
    packed, groups = call(
        pack_kernel,
        [shape_of(own_cells, ROWS, slots), shape_of(8, slots)],
        [pltpu.with_memory_space_constraint(x, pltpu.HBM) for x in operands],
        [pl.BlockSpec(memory_space=pltpu.HBM)] * 7,
        scratch=[pltpu.SMEM(operands[0].shape, jnp.int32)]
        + [pltpu.VMEM(x.shape, x.dtype) for x in operands[1:]]
        + [pltpu.SemaphoreType.DMA((7,))],
    )
    column = lax.all_gather(packed, "gy").reshape(cells, ROWS, slots)
    (beside,) = sideways(column, (0,))
    scratch = [
        pltpu.VMEM((cells, 2 * COMPS * NVEC, slots), BF16),
        pltpu.VMEM((cells, slots, 64), BF16),
        pltpu.VMEM((cells, slots, 64), F32),
    ]

    def pair_shapes(count):
        return [shape_of(count // 2, 4, slots, slots, dtype=BF16)] * 2

    fields_shape = shape_of(cells, 3 * NVEC, slots)
    begun, *own_pairs = call(
        own_pairs_kernel,
        [fields_shape] + pair_shapes(6),
        (column, groups),
        scratch=scratch + [pltpu.VMEM((6, slots, slots), F32)],
    )
    last_shape = shape_of(cells, 3, slots)
    partial, newest, *beside_pairs = call(
        beside_pairs_kernel,
        [fields_shape, last_shape] + pair_shapes(12),
        (column, beside, begun),
        scratch=scratch + [pltpu.VMEM((12, slots, slots), F32)],
    )
    newest_crossed, newest = sideways(newest, (1, 0))
    shared = lax.all_gather(partial, "gy")
    scratch = [pltpu.VMEM((cells, 2 * COMPS, slots), BF16)]
    jacobi, begun = call(
        own_apply_kernel, [last_shape, last_shape], (column, shared, *own_pairs), scratch=scratch
    )
    partial = call(
        beside_apply_kernel,
        last_shape,
        (column, beside, newest, newest_crossed, *beside_pairs, begun),
        scratch=scratch,
    )
    shared_last = lax.all_gather(partial, "gy")
    gram = call(
        gram_kernel,
        shape_of(2, 2 * NVEC * NVEC),
        (column, jacobi, shared, shared_last, past_res),
    )
    gram = jnp.sum(exchanged(gram, ("gx_1", "gy")), axis=0)
    partials = exchanged(gram, ("gx_0",))
    following, weights = call(
        finish_kernel,
        [shape_of(3, own_cells, slots), shape_of(1, NVEC)],
        (partials, column, jacobi, shared, shared_last),
    )
    return (jnp.swapaxes(following, 0, 1)[None], weights.reshape(NVEC))


def solution(mesh):
    torus = Mesh(
        mesh.devices.reshape(mesh.shape["box"], TORUS_Z, TORUS_X, mesh.shape["gy"]),
        ("box", "gx_0", "gx_1", "gy"),
    )
    return jax.shard_map(
        body,
        mesh=torus,
        in_specs=(
            P(BOX_GX, "gy", None, None),
            P(BOX_GX, "gy", None),
            P(BOX_GX, "gy", None),
            P(BOX_GX, "gy", None),
            P(BOX_GX, "gy", None, None),
            P(BOX_GX, "gy", None, None),
            P(BOX_GX, "gy", None, None, None),
            P(BOX_GX, "gy", None, None, None),
        ),
        out_specs=(P(BOX_GX, "gy", None, None), P("box")),
        check_vma=False,
    )
```
